32 devices in a mesh: azi: 8 (over z, core), ax: 2 (over y), rad: 2 (over x).
Axes of the slice: x: 2, y: 2, z: 4, core: 2. Of those that a mesh axis runs over, the one named last changes fastest.
Arguments:
- fields: float32 [2, 512, 32, 1024], P(None, 'azi', 'ax', 'rad'), may hold values from 0 to 1.5
- swirl_speed: float32 [512, 32, 1024], P('azi', 'ax', 'rad'), may hold values from 0.05 to 0.35
- ghost_mask: int32 [512, 32, 1024], P('azi', 'ax', 'rad'), may hold values 0 or 1
- tile_flags: int32 [32, 32], P('azi', 'ax'), may hold values 0 or 1
- outlet_gain: float32 [2, 32], replicated, may hold values from 0.25 to 1
- feed_rate: float32 [8, 8, 8], P('azi'), may hold values from 0.05 to 0.5
- plenum: float32 [8, 8, 8, 1024], P('azi', None, None, 'rad'), may hold values from 0.5 to 1.5
- feed_target: int32 [8, 8, 8], P('azi'), may hold values from -1 to 255, as said below
Outputs:
- new_fields: float32 [2, 512, 32, 1024], P(None, 'azi', 'ax', 'rad')
The draws below stay inside these ranges and needn't reach their ends.
Inputs may be any that keep to these rules, and one draw needn't show every extreme that they name: `feed_target`: entry i >= 0 names azimuthal cell i // 4 and axial cell i mod 4 of sector d; -1 marks an empty slot, and the used slots of a pair come first. At most 8 slots per pair are used; in every draw one sector receives 8 from every sector.
All inputs are finite; a program needn't handle non-finite values. No bound on the sum of `ghost_mask` or of `tile_flags` on one device may be relied on, other than what follows from the above.
Results may differ from the reference program's by a relative error of at most 0.00005.
Values sent between devices are 32-bit elements; how exact they have to be, the bound alone decides.
No kernel may reach another device: no remote copies, remote signals or barrier semaphores. Data moves between devices by JAX's collectives and lax.ppermute only.
A program may use at most 64 MiB of HBM per device.

```python
import math
import jax
import jax.numpy as jnp
from jax import lax

CT = 64
K = 32
TILE = 16
HEAD = 4
SLOTS = 8
NT = 512
NA = 32
NR = 1024
N_AZI = 8


def draw_feed_target(key, part):
    key_cap = jax.random.fold_in(key, 11)
    key_count = jax.random.fold_in(key, 12)
    key_full = jax.random.fold_in(key, 13)
    key_cells = jax.random.fold_in(key, 14)
    capacity = jax.random.randint(key_cap, (N_AZI,), 1, SLOTS + 1)
    counts = jax.random.randint(key_count, (N_AZI, N_AZI), 1, capacity[:, None] + 1)
    full_sector = jax.random.randint(key_full, (), 0, N_AZI)
    sector_ids = jnp.arange(N_AZI, dtype=jnp.int32)[:, None]
    counts = jnp.where(sector_ids == full_sector, SLOTS, counts)
    cells = jax.random.randint(key_cells, (N_AZI, N_AZI, SLOTS), 0, CT * HEAD)
    slot_ids = jnp.arange(SLOTS, dtype=jnp.int32)[None, None, :]
    return jnp.where(slot_ids < counts[:, :, None], cells, -1).astype(jnp.int32)


def with_ends(values, key, least, high):
    place = [jax.random.randint(jax.random.fold_in(key, axis), (), 0, length) for axis, length in enumerate(values.shape)]
    widest = values.shape.index(max(values.shape))
    next_to = place[:widest] + [(place[widest] + 1) % values.shape[widest]] + place[widest + 1:]
    return values.at[tuple(place)].set(least).at[tuple(next_to)].set(high)


def shard_levels(own_key, shape, split, smallest, high):
    factor_of = 1.0
    for axis_at, blocks in split:
        heights = jax.random.uniform(jax.random.fold_in(jax.random.fold_in(own_key, 6), axis_at), (blocks,), jnp.float32, smallest / len(split), high / len(split))
        factor_of = factor_of * jnp.repeat(jnp.exp(heights), shape[axis_at] // blocks).reshape((-1,) + (1,) * (len(shape) - 1 - axis_at))
    return factor_of


def setup_inputs(seed: int = 0) -> dict:
    key_of = jax.random.split(jax.random.key(seed), 9)
    fields = jnp.clip(1.5 * jax.random.uniform(key_of[0], (2, NT, NA, NR), jnp.float32) ** shard_levels(key_of[0], (2, NT, NA, NR), ((1, 8), (2, 2), (3, 2)), -0.2, 0.2), 0.0, 1.5)
    swirl_speed = jnp.clip(0.05 + 0.29999999 * jax.random.uniform(key_of[1], (NT, NA, NR), jnp.float32) ** shard_levels(key_of[1], (NT, NA, NR), ((0, 8), (1, 2), (2, 2)), -0.2, 0.2), 0.05, 0.35)
    ghost_mask = with_ends((jax.random.randint(key_of[2], (NT, NA, NR), 0, 4) < 1).astype(jnp.int32), jax.random.fold_in(key_of[2], 1), 0, 1)
    tile_flags = with_ends((jax.random.randint(key_of[3], (NT // TILE, NA), 0, 2) < 1).astype(jnp.int32), jax.random.fold_in(key_of[3], 1), 0, 1)
    outlet_gain = jnp.clip(jnp.exp(jax.random.uniform(key_of[4], (2, K), jnp.float32, math.log(0.25), math.log(1.0))), 0.25, 1.0)
    feed_rate = jnp.clip(jnp.exp(math.log(0.5) - 2.3025851 * jax.random.uniform(key_of[5], (N_AZI, N_AZI, SLOTS), jnp.float32) ** shard_levels(key_of[5], (N_AZI, N_AZI, SLOTS), ((0, 8),), -0.2, 0.2)), 0.05, 0.5)
    plenum = jnp.clip(0.5 + 1.0 * jax.random.uniform(key_of[6], (N_AZI, N_AZI, SLOTS, NR), jnp.float32) ** shard_levels(key_of[6], (N_AZI, N_AZI, SLOTS, NR), ((0, 8), (3, 2)), -0.2, 0.2), 0.5, 1.5)
    feed_target = draw_feed_target(jax.random.fold_in(key_of[8], 71), 0)
    return {"fields": fields, "swirl_speed": swirl_speed, "ghost_mask": ghost_mask, "tile_flags": tile_flags, "outlet_gain": outlet_gain, "feed_rate": feed_rate, "plenum": plenum, "feed_target": feed_target}


def phase_table(length, first_cell, cell_count, mode_count):
    theta_index = first_cell + jnp.arange(cell_count, dtype=jnp.int32)
    mode_order = jnp.arange(1, mode_count + 1, dtype=jnp.int32)
    phase_int = mode_order[:, None] * theta_index[None, :] % length
    angles = phase_int.astype(jnp.float32) * (2.0 * math.pi / length)
    return jnp.concatenate([jnp.cos(angles), jnp.sin(angles)], axis=0)

def reference(fields, swirl_speed, ghost_mask, tile_flags, outlet_gain, feed_rate, plenum, feed_target):
    length = fields.shape[1]
    depth_cells = fields.shape[2]
    radial_cells = fields.shape[3]
    phase_rows = phase_table(length, 0, length, K)
    outlet_plane = fields[:, :, -1, :]
    mode_sums = jnp.einsum('mt,ctr->cmr', phase_rows, outlet_plane, precision=lax.Precision.HIGHEST)
    gain_both = jnp.concatenate([outlet_gain, outlet_gain], axis=1)
    rebuilt = jnp.einsum('mt,cmr->ctr', phase_rows, mode_sums * gain_both[:, :, None], precision=lax.Precision.HIGHEST)
    ghost_plane = outlet_plane - rebuilt * (2.0 / math.sqrt(K * length))
    zero_axial = jnp.zeros((2, length, 1, radial_cells), jnp.float32)
    zero_radial = jnp.zeros((2, length, depth_cells, 1), jnp.float32)
    axial_next = jnp.concatenate([fields[:, :, 1:, :], ghost_plane[:, :, None, :]], axis=2)
    axial_prev = jnp.concatenate([zero_axial, fields[:, :, :-1, :]], axis=2)
    radial_next = jnp.concatenate([fields[:, :, :, 1:], zero_radial], axis=3)
    radial_prev = jnp.concatenate([zero_radial, fields[:, :, :, :-1]], axis=3)
    theta_prev = jnp.roll(fields, 1, axis=1)
    theta_next = jnp.roll(fields, -1, axis=1)
    laplace_term = theta_prev + theta_next + axial_prev + axial_next + radial_prev + radial_next - 6.0 * fields
    upwind_term = swirl_speed[None] * (fields - theta_prev)
    energy = fields[0]
    fuel_part = fields[1]
    tile_on = jnp.repeat(tile_flags, TILE, axis=0).astype(jnp.float32)
    inert = ghost_mask.astype(jnp.float32)
    reaction = 0.5 * tile_on[:, :, None] * (1.0 - inert) * fuel_part * jax.nn.sigmoid(4.0 * (energy - 0.5))
    payload = feed_rate[:, :, :, None] * plenum
    payload = jnp.transpose(payload, (1, 0, 2, 3))
    sector_ids = jnp.arange(N_AZI, dtype=jnp.int32)[:, None, None]
    occupied = feed_target >= 0
    theta_rows = jnp.where(occupied, sector_ids * CT + feed_target // HEAD, length).astype(jnp.int32)
    axial_rows = jnp.where(occupied, feed_target % HEAD, 0).astype(jnp.int32)
    feed_term = jnp.zeros((length, depth_cells, radial_cells), jnp.float32)
    feed_term = feed_term.at[theta_rows.reshape(-1), axial_rows.reshape(-1)].add(payload.reshape(-1, radial_cells), mode='drop')
    new_energy = energy - upwind_term[0] + 0.1 * laplace_term[0] + 2.0 * reaction
    new_fuel = fuel_part - upwind_term[1] + 0.1 * laplace_term[1] - reaction + feed_term
    return jnp.stack([new_energy, new_fuel], axis=0)
```

```python
import functools
import math

import jax
import jax.numpy as jnp
from jax import lax
from jax.experimental import pallas as pl
from jax.experimental.pallas import tpu as pltpu
from jax.sharding import PartitionSpec as P

TILE = 16
HEAD = 4
LANES = 128
SUB = 8
HIGH = lax.Precision.HIGHEST
VMEM = pl.BlockSpec(memory_space=pltpu.VMEM)
SMEM = pl.BlockSpec(memory_space=pltpu.SMEM)
HBM = pl.BlockSpec(memory_space=pltpu.HBM)
f32 = jnp.float32


def params(mib):
    return pltpu.CompilerParams(vmem_limit_bytes=mib << 20)


def cost(flops, size):
    return pl.CostEstimate(flops=flops, bytes_accessed=size, transcendentals=0)


def phases(length, first_cell, cell_count, mode_count):
    cells = first_cell + jnp.arange(cell_count, dtype=jnp.int32)
    order = jnp.arange(1, mode_count + 1, dtype=jnp.int32)
    angle = (order[:, None] * cells[None, :] % length).astype(f32) * (2.0 * math.pi / length)
    turned = (cells[:, None] * order[None, :] % length).astype(f32) * (2.0 * math.pi / length)
    return (
        jnp.concatenate([jnp.cos(angle), jnp.sin(angle)], axis=0),
        jnp.concatenate([jnp.cos(turned), jnp.sin(turned)], axis=1),
    )


def prepare(
    chunk, fields, phase, rate, plenum, keep, send, shift, row_top, row_out, column, local, tile, sem
):
    azi, ax, rad = lax.axis_index("azi"), lax.axis_index("ax"), lax.axis_index("rad")
    last_ax = lax.axis_size("ax") - 1
    count, cells, depth, width = fields.shape
    sectors = plenum.shape[0]
    slots = plenum.shape[1]
    pairs = sectors // 2
    parity, place = azi % 2, azi // 2
    base = pairs * chunk
    t_pair = jnp.where(parity == 0, cells - 1, 0)
    t_shift = jnp.where(parity == 0, 0, cells - 1)
    row_sent = jnp.where(ax == 0, depth - 1, 0)
    side = jnp.where(rad == 0, width - LANES, 0)
    first = pltpu.make_async_copy(fields.at[:, :, depth - 1, :], row_top, sem.at[0])
    first.start()
    copies = []
    for c in range(count):
        rows = slice(base + c * depth, base + (c + 1) * depth)
        copies.append(pltpu.make_async_copy(fields.at[c, t_pair], send.at[rows], sem.at[1 + 2 * c]))
        rows = slice(c * depth, (c + 1) * depth)
        copies.append(pltpu.make_async_copy(fields.at[c, t_shift], shift.at[rows], sem.at[2 + 2 * c]))
    edge = pltpu.make_async_copy(
        fields.at[:, :, :, pl.ds(pl.multiple_of(side, LANES), LANES)], tile, sem.at[1 + 2 * count]
    )
    for one in copies:
        one.start()
    edge.start()
    face = pltpu.make_async_copy(fields.at[:, :, row_sent, :], row_out, sem.at[2 + 2 * count])
    face.start()
    whole = pltpu.make_async_copy(fields, local, sem.at[3 + 2 * count])
    whole.start()

    @pl.when(ax == last_ax)
    def _():
        first.wait()
        sums = [
            jnp.dot(phase[...], row_top[c], precision=HIGH, preferred_element_type=f32)
            for c in range(count)
        ]
        modes = phase.shape[0]
        length = count * modes // sectors
        blocks = []
        for s in range(sectors):
            c, m = divmod(s * length, modes)
            blocks.append(sums[c][m : m + length])
        for q in range(pairs):
            even, odd = blocks[2 * q], blocks[2 * q + 1]
            at = pl.multiple_of((q ^ place) * chunk, SUB)
            keep[pl.ds(at, length)] = jnp.where(parity == 0, even, odd)
            send[pl.ds(at, length)] = jnp.where(parity == 0, odd, even)
            if chunk > length:
                rest = pl.multiple_of(at + length, SUB)
                keep[pl.ds(rest, chunk - length)] = jnp.zeros((chunk - length, width), f32)
                send[pl.ds(rest, chunk - length)] = jnp.zeros((chunk - length, width), f32)

    @pl.when(ax != last_ax)
    def _():
        first.wait()
        for q in range(pairs):
            at = pl.multiple_of((q ^ place) * chunk, SUB)
            even = rate[2 * q] * plenum[2 * q]
            odd = rate[2 * q + 1] * plenum[2 * q + 1]
            own = jnp.where(parity == 0, even, odd)
            other = jnp.where(parity == 0, odd, even)
            for p in range(2):
                rows = pl.ds(pl.multiple_of(at + p * slots, SUB), slots)
                keep[rows] = jnp.where(parity == p, own, 0.0)
                send[rows] = jnp.where(parity == p, other, 0.0)
            if chunk > 2 * slots:
                rest = pl.ds(pl.multiple_of(at + 2 * slots, SUB), chunk - 2 * slots)
                keep[rest] = jnp.zeros((chunk - 2 * slots, width), f32)
                send[rest] = jnp.zeros((chunk - 2 * slots, width), f32)

    edge.wait()
    lane = lax.broadcasted_iota(jnp.int32, (SUB, LANES), 1)
    halves = depth // SUB
    source = jnp.where(rad == 0, LANES - 1, 0)
    for g in range(column.shape[0]):
        acc = jnp.zeros((SUB, LANES), f32)
        for j in range(LANES):
            c, rest = divmod(g * LANES + j, cells * halves)
            t, h = divmod(rest, halves)
            piece = tile[c, t, h * SUB : (h + 1) * SUB, :]
            turned = pltpu.roll(piece, jnp.where(rad == 0, (j + 1) % LANES, j), 1)
            acc = jnp.where(lane == j, turned, acc)
        column[g] = acc
    for one in copies:
        one.wait()
    face.wait()
    whole.wait()


def stencil(fields, swirl, mask, tiles, near, shift, column, out):
    azi, rad = lax.axis_index("azi"), lax.axis_index("rad")
    last_rad = lax.axis_size("rad") - 1
    count, cells, depth, width = fields.shape
    base = near.shape[0] - count * depth
    parity = azi % 2
    halves = depth // SUB
    blocks = width // LANES
    lane = lax.broadcasted_iota(jnp.int32, (depth, LANES), 1)
    row = lax.broadcasted_iota(jnp.int32, (depth, LANES), 0)
    at_left, at_right = lane == 0, lane == LANES - 1
    at_low, at_high = row == 0, row == depth - 1

    def slab(t, before, after):
        tile_row = tiles[t // TILE]
        x, s, prev = [], [], []
        for c in range(count):
            parts = [fields[c, t, :, l * LANES : (l + 1) * LANES] for l in range(blocks)]
            edge_low, edge_high = [], []
            for h in range(halves):
                n = (c * cells + t) * halves + h
                g, j = n // LANES, n % LANES
                values = column[g]
                edge_low.append(pltpu.roll(values, (LANES - j) % LANES, 1))
                edge_high.append(pltpu.roll(values, LANES - 1 - j, 1))
            left_edge = jnp.where(rad > 0, jnp.concatenate(edge_low, axis=0), 0.0)
            right_edge = jnp.where(rad < last_rad, jnp.concatenate(edge_high, axis=0), 0.0)
            ups = [pltpu.roll(v, 1, 1) for v in parts]
            downs = [pltpu.roll(v, LANES - 1, 1) for v in parts]
            total, previous = [], []
            for l in range(blocks):
                left = jnp.where(at_left, ups[l - 1] if l else left_edge, ups[l])
                right = jnp.where(at_right, downs[l + 1] if l + 1 < blocks else right_edge, downs[l])
                low = jnp.where(at_low, 0.0, pltpu.roll(parts[l], 1, 0))
                high = jnp.where(at_high, 0.0, pltpu.roll(parts[l], depth - 1, 0))
                total.append((left + right) + (low + high) + after(c, l))
                previous.append(before(c, l))
            x.append(parts)
            s.append(total)
            prev.append(previous)
        for l in range(blocks):
            lanes = slice(l * LANES, (l + 1) * LANES)
            speed = swirl[t, :, lanes]
            inert = mask[t, :, lanes].astype(f32)
            energy, fuel = x[0][l], x[1][l]
            burn = tile_row * (1.0 - inert) * fuel * (1.0 + jnp.tanh(2.0 * energy - 1.0))
            stay, come = 0.4 - speed, speed + 0.1
            out[0, t, :, lanes] = energy * stay + 0.1 * s[0][l] + come * prev[0][l] + 2.0 * burn
            out[1, t, :, lanes] = fuel * stay + 0.1 * s[1][l] + come * prev[1][l] - burn

    def halo(use_near):
        def value(c, l):
            lanes = slice(l * LANES, (l + 1) * LANES)
            a = near[base + c * depth : base + (c + 1) * depth, lanes]
            b = shift[c * depth : (c + 1) * depth, lanes]
            return jnp.where(use_near, a, b)

        return value

    def inside(t):
        return lambda c, l: fields[c, t, :, l * LANES : (l + 1) * LANES]

    slab(0, halo(parity == 1), inside(1))

    def step(t, carry):
        slab(t, inside(t - 1), inside(t + 1))
        return carry

    lax.fori_loop(1, cells - 1, step, 0)
    slab(cells - 1, inside(cells - 2), halo(parity == 0))


def feed_rows(chunk, slots, targets, *refs):
    *arrived, feed = refs
    place = lax.axis_index("azi") // 2
    rows = feed.shape[0] - SUB
    feed[...] = jnp.zeros(feed.shape, f32)

    @pl.when(lax.axis_index("ax") == 0)
    def _():
        for k, block in enumerate(arrived):
            for p in range(2):
                for j in range(slots):
                    target = targets[2 * (place ^ k) + p, j]
                    at = jnp.where(target >= 0, target // HEAD * SUB + target % HEAD, rows)
                    r = p * slots + j
                    feed[pl.ds(at, 1), :] += block[r : r + 1, :]


def finish(chunk, length, axial, row_top, own, other, weights, feed, before, out, modes, high, result, sem):
    azi, ax = lax.axis_index("azi"), lax.axis_index("ax")
    last_ax = lax.axis_size("ax") - 1
    count, cells, depth, width = before.shape
    parity, place = azi % 2, azi // 2
    pairs = own.shape[0] // chunk

    @pl.when(ax == last_ax)
    def _():
        for k in range(pairs):
            for ref, p in ((own, parity), (other, 1 - parity)):
                at = pl.multiple_of((2 * (place ^ k) + p) * length, SUB)
                modes[pl.ds(at, length)] = ref[k * chunk : k * chunk + length]
        per = modes.shape[0] // count
        for c in range(count):
            rebuilt = jnp.dot(
                weights[c], modes[c * per : (c + 1) * per], precision=HIGH, preferred_element_type=f32
            )
            high[c] = 0.1 * row_top[c] - rebuilt

    @pl.when(ax != last_ax)
    def _():
        for c in range(count):
            high[c] = 0.1 * axial[c]

    scale = jnp.where(ax > 0, 0.1, 0.0)
    row = lax.broadcasted_iota(jnp.int32, (SUB, width), 0)
    group = SUB
    copies = []
    for b in range(cells // group):
        for c in range(count):
            low_rows = scale * axial[c, b * group : (b + 1) * group]
            high_rows = high[c, b * group : (b + 1) * group]
            for i in range(group):
                t = b * group + i
                head = before[c, t, :SUB] + jnp.where(row == 0, low_rows[i : i + 1], 0.0)
                if c == 1:
                    head = head + feed[t * SUB : (t + 1) * SUB]
                result[c, t, :SUB] = head
                if depth > 2 * SUB:
                    result[c, t, SUB : depth - SUB] = before[c, t, SUB : depth - SUB]
                tail = before[c, t, depth - SUB :]
                result[c, t, depth - SUB :] = tail + jnp.where(row == SUB - 1, high_rows[i : i + 1], 0.0)
            cells_at = pl.ds(b * group, group)
            copy = pltpu.make_async_copy(result.at[c, cells_at], out.at[c, cells_at], sem.at[c, b])
            copy.start()
            copies.append(copy)
    for copy in copies:
        copy.wait()


def body(fields, swirl_speed, ghost_mask, tile_flags, outlet_gain, feed_rate, plenum, feed_target):
    sectors, slabs, radials = lax.axis_size("azi"), lax.axis_size("ax"), lax.axis_size("rad")
    count, cells, depth, width = fields.shape
    half_modes = outlet_gain.shape[1]
    modes = 2 * half_modes
    slots = plenum.shape[2]
    length = count * modes // sectors
    chunk = max(length, 2 * slots)
    pairs = sectors // 2
    total_cells = cells * sectors
    phase, phase_t = phases(total_cells, lax.axis_index("azi") * cells, cells, half_modes)
    gain = jnp.concatenate([outlet_gain, outlet_gain], axis=1)
    weights = phase_t[None] * gain[:, None, :] * (0.1 * 2.0 / math.sqrt(half_modes * total_cells))
    rate = jnp.broadcast_to(feed_rate[0][:, :, None], (sectors, slots, width))
    tiles = jnp.broadcast_to(0.25 * tile_flags.astype(f32)[:, :, None], tile_flags.shape + (LANES,))
    groups = count * cells * depth // SUB // LANES

    struct = jax.ShapeDtypeStruct
    keep, send, shift, row_top, row_out, column, local = pl.pallas_call(
        functools.partial(prepare, chunk),
        out_shape=(
            struct((pairs * chunk, width), f32),
            struct((pairs * chunk + count * depth, width), f32),
            struct((count * depth, width), f32),
            struct((count, cells, width), f32),
            struct((count, cells, width), f32),
            struct((groups, SUB, LANES), f32),
            struct(fields.shape, f32),
        ),
        in_specs=[HBM, VMEM, VMEM, VMEM],
        out_specs=[VMEM] * 7,
        scratch_shapes=[
            pltpu.VMEM((count, cells, depth, LANES), f32),
            pltpu.SemaphoreType.DMA((2 * count + 4,)),
        ],
        compiler_params=params(12),
        cost_estimate=cost(1 << 26, 1 << 21),
        name="prepare",
    )(pltpu.with_memory_space_constraint(fields, pltpu.HBM), phase, rate, plenum[0])

    def swap(x, k):
        return lax.ppermute(x, "azi", [(i, i ^ k) for i in range(sectors)])

    near = swap(send, 1)
    offset = [(i, (i + 1) % sectors if i % 2 else (i - 1) % sectors) for i in range(sectors)]
    far = lax.ppermute(shift, "azi", offset)
    axial = lax.ppermute(row_out, "ax", [(0, 1), (1, 0)])
    edge = lax.ppermute(column, "rad", [(0, 1), (1, 0)])

    mixed = keep + near[: pairs * chunk]
    parts = [mixed[k * chunk : (k + 1) * chunk] for k in range(pairs)]
    arrived = [parts[0]] + [swap(parts[k], 2 * k) for k in range(1, pairs)]
    summed = functools.reduce(jnp.add, arrived)

    before = pl.pallas_call(
        stencil,
        out_shape=struct(fields.shape, f32),
        in_specs=[VMEM] * 7,
        out_specs=VMEM,
        compiler_params=params(12),
        cost_estimate=cost(1 << 28, 1 << 23),
        name="stencil",
    )(local, swirl_speed, ghost_mask, tiles, near, far, edge)

    feed = pl.pallas_call(
        functools.partial(feed_rows, chunk, slots),
        out_shape=struct((cells * SUB + SUB, width), f32),
        in_specs=[SMEM] + [VMEM] * pairs,
        out_specs=VMEM,
        compiler_params=params(8),
        cost_estimate=cost(1 << 25, 1 << 20),
        name="feed",
    )(feed_target[0], *arrived)

    gathered = jnp.concatenate([summed] + [swap(summed, 2 * k) for k in range(1, pairs)], axis=0)
    other = swap(gathered, 1)

    return pl.pallas_call(
        functools.partial(finish, chunk, length),
        out_shape=struct(fields.shape, f32),
        in_specs=[VMEM] * 7,
        out_specs=HBM,
        scratch_shapes=[
            pltpu.VMEM((count * modes, width), f32),
            pltpu.VMEM((count, cells, width), f32),
            pltpu.VMEM(fields.shape, f32),
            pltpu.SemaphoreType.DMA((count, cells // SUB)),
        ],
        compiler_params=params(16),
        cost_estimate=cost(1 << 26, 1 << 23),
        name="finish",
    )(axial, row_top, gathered, other, weights, feed, before)


def solution(mesh):
    return jax.shard_map(
        body,
        mesh=mesh,
        in_specs=(
            P(None, "azi", "ax", "rad"),
            P("azi", "ax", "rad"),
            P("azi", "ax", "rad"),
            P("azi", "ax"),
            P(),
            P("azi", None, None),
            P("azi", None, None, "rad"),
            P("azi", None, None),
        ),
        out_specs=P(None, "azi", "ax", "rad"),
        check_vma=False,
    )
```

```python
import functools
import math

import jax
import jax.numpy as jnp
from jax import lax
from jax.experimental import pallas as pl
from jax.experimental.pallas import tpu as pltpu
from jax.sharding import PartitionSpec as P


TILE = 16
HEAD = 4
LANES = 128
SUB = 8
HIGH = lax.Precision.HIGHEST
VMEM = pl.BlockSpec(memory_space=pltpu.VMEM)
SMEM = pl.BlockSpec(memory_space=pltpu.SMEM)
HBM = pl.BlockSpec(memory_space=pltpu.HBM)
f32 = jnp.float32


def params(mib):
    return pltpu.CompilerParams(vmem_limit_bytes=mib << 20)


def cost(flops, size):
    return pl.CostEstimate(flops=flops, bytes_accessed=size, transcendentals=0)


def in_hbm(x):
    return pltpu.with_memory_space_constraint(x, pltpu.HBM)


def phases(length, first_cell, cell_count, mode_count):
    cells = first_cell + jnp.arange(cell_count, dtype=jnp.int32)
    order = jnp.arange(1, mode_count + 1, dtype=jnp.int32)
    angle = (order[:, None] * cells[None, :] % length).astype(f32) * (2.0 * math.pi / length)
    turned = (cells[:, None] * order[None, :] % length).astype(f32) * (2.0 * math.pi / length)
    return (
        jnp.concatenate([jnp.cos(angle), jnp.sin(angle)], axis=0),
        jnp.concatenate([jnp.cos(turned), jnp.sin(turned)], axis=1),
    )


def prepare(
    chunk, fields, phase, rate, profile, keep, send, shift, row_top, row_out, column, plenum, tile, sem
):
    azi, ax, rad = lax.axis_index("azi"), lax.axis_index("ax"), lax.axis_index("rad")
    last_ax = lax.axis_size("ax") - 1
    count, cells, depth, width = fields.shape
    sectors, slots, _ = profile.shape
    pairs = sectors // 2
    parity, place = azi % 2, azi // 2
    base = pairs * chunk
    t_pair = jnp.where(parity == 0, cells - 1, 0)
    t_shift = jnp.where(parity == 0, 0, cells - 1)
    row_sent = jnp.where((ax == 0) & (last_ax == 1), depth - 1, 0)
    if lax.axis_size("rad") == 2:
        sides = [(jnp.where(rad == 0, width - LANES, 0), jnp.where(rad == 0, LANES - 1, 0))]
    else:
        sides = [(width - LANES, LANES - 1), (0, 0)]
    first = pltpu.make_async_copy(fields.at[:, :, depth - 1, :], row_top, sem.at[0])
    first.start()
    copies = []
    for c in range(count):
        rows = slice(base + c * depth, base + (c + 1) * depth)
        copies.append(pltpu.make_async_copy(fields.at[c, t_pair], send.at[rows], sem.at[1 + 2 * c]))
        rows = slice(c * depth, (c + 1) * depth)
        copies.append(pltpu.make_async_copy(fields.at[c, t_shift], shift.at[rows], sem.at[2 + 2 * c]))
    edges = [
        pltpu.make_async_copy(
            fields.at[:, :, :, pl.ds(pl.multiple_of(side, LANES), LANES)], tile.at[e], sem.at[4 + 2 * count + e]
        )
        for e, (side, _) in enumerate(sides)
    ]
    for one in copies:
        one.start()
    for edge in edges:
        edge.start()
    face = pltpu.make_async_copy(fields.at[:, :, row_sent, :], row_out, sem.at[2 + 2 * count])
    face.start()
    supply = pltpu.make_async_copy(profile, plenum, sem.at[3 + 2 * count])
    supply.start()

    @pl.when(ax == last_ax)
    def _():
        first.wait()
        supply.wait()
        sums = [
            jnp.dot(phase[...], row_top[c], precision=HIGH, preferred_element_type=f32)
            for c in range(count)
        ]
        modes = phase.shape[0]
        length = count * modes // sectors
        blocks = []
        for s in range(sectors):
            c, m = divmod(s * length, modes)
            blocks.append(sums[c][m : m + length])
        for q in range(pairs):
            even, odd = blocks[2 * q], blocks[2 * q + 1]
            at = q * chunk
            keep[at : at + length] = jnp.where(parity == 0, even, odd)
            send[at : at + length] = jnp.where(parity == 0, odd, even)
            if chunk > length:
                keep[at + length : at + chunk] = jnp.zeros((chunk - length, width), f32)
                send[at + length : at + chunk] = jnp.zeros((chunk - length, width), f32)

    @pl.when(ax != last_ax)
    def _():
        first.wait()
        supply.wait()
        turned = rate[...].T
        for q in range(pairs):
            at = pl.multiple_of((q ^ place) * chunk, SUB)
            even = turned[:, 2 * q : 2 * q + 1] * plenum[2 * q]
            odd = turned[:, 2 * q + 1 : 2 * q + 2] * plenum[2 * q + 1]
            own = jnp.where(parity == 0, even, odd)
            other = jnp.where(parity == 0, odd, even)
            for p in range(2):
                rows = pl.ds(pl.multiple_of(at + p * slots, SUB), slots)
                keep[rows] = jnp.where(parity == p, own, 0.0)
                send[rows] = jnp.where(parity == p, other, 0.0)
            if chunk > 2 * slots:
                rest = pl.ds(pl.multiple_of(at + 2 * slots, SUB), chunk - 2 * slots)
                keep[rest] = jnp.zeros((chunk - 2 * slots, width), f32)
                send[rest] = jnp.zeros((chunk - 2 * slots, width), f32)

    lane = lax.broadcasted_iota(jnp.int32, (SUB, LANES), 1)
    halves = depth // SUB
    for e, (_, source) in enumerate(sides):
        edges[e].wait()
        for g in range(column.shape[1]):
            acc = jnp.zeros((SUB, LANES), f32)
            for j in range(LANES):
                c, rest = divmod(g * LANES + j, cells * halves)
                t, h = divmod(rest, halves)
                piece = tile[e, c, t, h * SUB : (h + 1) * SUB, :]
                acc = jnp.where(lane == j, pltpu.roll(piece, (j - source) % LANES, 1), acc)
            column[e, g] = acc
    for one in copies:
        one.wait()
    face.wait()


def stencil(fields, swirl, mask, tiles, near, shift, column_low, column_high, out):
    azi, rad = lax.axis_index("azi"), lax.axis_index("rad")
    last_rad = lax.axis_size("rad") - 1
    count, cells, depth, width = fields.shape
    base = near.shape[0] - count * depth
    parity = azi % 2
    halves = depth // SUB
    blocks = width // LANES
    lane = lax.broadcasted_iota(jnp.int32, (depth, LANES), 1)
    row = lax.broadcasted_iota(jnp.int32, (depth, LANES), 0)
    at_left, at_right = lane == 0, lane == LANES - 1
    at_low, at_high = row == 0, row == depth - 1

    def slab(t, before, after):
        tile_row = tiles[t // TILE]
        x, s, prev = [], [], []
        for c in range(count):
            parts = [fields[c, t, :, l * LANES : (l + 1) * LANES] for l in range(blocks)]
            edge_low, edge_high = [], []
            for h in range(halves):
                n = (c * cells + t) * halves + h
                g, j = n // LANES, n % LANES
                edge_low.append(pltpu.roll(column_low[g], (LANES - j) % LANES, 1))
                edge_high.append(pltpu.roll(column_high[g], LANES - 1 - j, 1))
            left_edge = jnp.where(rad > 0, jnp.concatenate(edge_low, axis=0), 0.0)
            right_edge = jnp.where(rad < last_rad, jnp.concatenate(edge_high, axis=0), 0.0)
            ups = [pltpu.roll(v, 1, 1) for v in parts]
            downs = [pltpu.roll(v, LANES - 1, 1) for v in parts]
            total, previous = [], []
            for l in range(blocks):
                left = jnp.where(at_left, ups[l - 1] if l else left_edge, ups[l])
                right = jnp.where(at_right, downs[l + 1] if l + 1 < blocks else right_edge, downs[l])
                low = jnp.where(at_low, 0.0, pltpu.roll(parts[l], 1, 0))
                high = jnp.where(at_high, 0.0, pltpu.roll(parts[l], depth - 1, 0))
                total.append((left + right) + (low + high) + after(c, l))
                previous.append(before(c, l))
            x.append(parts)
            s.append(total)
            prev.append(previous)
        for l in range(blocks):
            lanes = slice(l * LANES, (l + 1) * LANES)
            speed = swirl[t, :, lanes]
            inert = mask[t, :, lanes].astype(f32)
            energy, fuel = x[0][l], x[1][l]
            burn = tile_row * (1.0 - inert) * fuel * (1.0 + jnp.tanh(2.0 * energy - 1.0))
            stay, come = 0.4 - speed, speed + 0.1
            out[0, t, :, lanes] = energy * stay + 0.1 * s[0][l] + come * prev[0][l] + 2.0 * burn
            out[1, t, :, lanes] = fuel * stay + 0.1 * s[1][l] + come * prev[1][l] - burn

    def halo(use_near):
        def value(c, l):
            lanes = slice(l * LANES, (l + 1) * LANES)
            a = near[base + c * depth : base + (c + 1) * depth, lanes]
            b = shift[c * depth : (c + 1) * depth, lanes]
            return jnp.where(use_near, a, b)

        return value

    def inside(t):
        return lambda c, l: fields[c, t, :, l * LANES : (l + 1) * LANES]

    slab(0, halo(parity == 1), inside(1))

    def step(t, carry):
        slab(t, inside(t - 1), inside(t + 1))
        return carry

    lax.fori_loop(1, cells - 1, step, 0)
    slab(cells - 1, inside(cells - 2), halo(parity == 0))


def feed_rows(slots, targets, *refs):
    *arrived, feed = refs
    place = lax.axis_index("azi") // 2
    rows = feed.shape[0] - SUB
    feed[...] = jnp.zeros(feed.shape, f32)

    @pl.when(lax.axis_index("ax") == 0)
    def _():
        for k, block in enumerate(arrived):
            for p in range(2):
                for j in range(slots):
                    target = targets[2 * (place ^ k) + p, j]
                    at = jnp.where(target >= 0, target // HEAD * SUB + target % HEAD, rows)
                    r = p * slots + j
                    feed[pl.ds(at, 1), :] += block[r : r + 1, :]


def finish(chunk, length, axial_low, axial_high, row_top, own, other, weights, feed, before, out, modes, high, result, sem):
    azi, ax = lax.axis_index("azi"), lax.axis_index("ax")
    last_ax = lax.axis_size("ax") - 1
    count, cells, depth, width = before.shape
    parity = azi % 2
    pairs = own.shape[0] // chunk

    @pl.when(ax == last_ax)
    def _():
        for k in range(pairs):
            for ref, p in ((own, parity), (other, 1 - parity)):
                at = pl.multiple_of((2 * k + p) * length, SUB)
                modes[pl.ds(at, length)] = ref[k * chunk : k * chunk + length]
        per = modes.shape[0] // count
        for c in range(count):
            rebuilt = jnp.dot(
                weights[c], modes[c * per : (c + 1) * per], precision=HIGH, preferred_element_type=f32
            )
            high[c] = 0.1 * row_top[c] - rebuilt

    @pl.when(ax != last_ax)
    def _():
        for c in range(count):
            high[c] = 0.1 * axial_high[c]

    scale = jnp.where(ax > 0, 0.1, 0.0)
    row = lax.broadcasted_iota(jnp.int32, (SUB, width), 0)
    group = SUB
    copies = []
    for b in range(cells // group):
        for c in range(count):
            low_rows = scale * axial_low[c, b * group : (b + 1) * group]
            high_rows = high[c, b * group : (b + 1) * group]
            for i in range(group):
                t = b * group + i
                head = before[c, t, :SUB] + jnp.where(row == 0, low_rows[i : i + 1], 0.0)
                if c == 1:
                    head = head + feed[t * SUB : (t + 1) * SUB]
                result[c, t, :SUB] = head
                if depth > 2 * SUB:
                    result[c, t, SUB : depth - SUB] = before[c, t, SUB : depth - SUB]
                tail = before[c, t, depth - SUB :]
                result[c, t, depth - SUB :] = tail + jnp.where(row == SUB - 1, high_rows[i : i + 1], 0.0)
            cells_at = pl.ds(b * group, group)
            copy = pltpu.make_async_copy(result.at[c, cells_at], out.at[c, cells_at], sem.at[c, b])
            copy.start()
            copies.append(copy)
    for copy in copies:
        copy.wait()


def body(fields, swirl_speed, ghost_mask, tile_flags, outlet_gain, feed_rate, plenum, feed_target):
    sectors, radials = lax.axis_size("azi"), lax.axis_size("rad")
    count, cells, depth, width = fields.shape
    half_modes = outlet_gain.shape[1]
    modes = 2 * half_modes
    slots = plenum.shape[2]
    length = count * modes // sectors
    chunk = max(length, 2 * slots)
    pairs = sectors // 2
    total_cells = cells * sectors
    phase, phase_t = phases(total_cells, lax.axis_index("azi") * cells, cells, half_modes)
    gain = jnp.concatenate([outlet_gain, outlet_gain], axis=1)
    weights = phase_t[None] * gain[:, None, :] * (0.1 * 2.0 / math.sqrt(half_modes * total_cells))
    tiles = jnp.broadcast_to(0.25 * tile_flags.astype(f32)[:, :, None], tile_flags.shape + (LANES,))
    groups = count * cells * depth // SUB // LANES

    struct = jax.ShapeDtypeStruct
    keep, send, shift, row_top, row_out, column = pl.pallas_call(
        functools.partial(prepare, chunk),
        out_shape=(
            struct((pairs * chunk, width), f32),
            struct((pairs * chunk + count * depth, width), f32),
            struct((count * depth, width), f32),
            struct((count, cells, width), f32),
            struct((count, cells, width), f32),
            struct((1 if radials == 2 else 2, groups, SUB, LANES), f32),
        ),
        in_specs=[HBM, VMEM, VMEM, HBM],
        out_specs=[VMEM] * 6,
        scratch_shapes=[
            pltpu.VMEM((sectors, slots, width), f32),
            pltpu.VMEM((1 if radials == 2 else 2, count, cells, depth, LANES), f32),
            pltpu.SemaphoreType.DMA((2 * count + 6,)),
        ],
        compiler_params=params(12),
        cost_estimate=cost(1 << 26, 1 << 21),
        name="prepare",
    )(in_hbm(fields), phase, feed_rate[0], in_hbm(plenum[0]))

    def swap(x, k):
        return lax.ppermute(x, "azi", [(i, i ^ k) for i in range(sectors)])

    def across(axis, to_high, to_low, to_only):
        size = lax.axis_size(axis)
        if size == 2:
            received = lax.ppermute(to_only, axis, [(0, 1), (1, 0)])
            return received, received
        ups = [(i, i + 1) for i in range(size - 1)]
        return lax.ppermute(to_high, axis, ups), lax.ppermute(to_low, axis, [(b, a) for a, b in ups])

    offset = [(i, (i + 1) % sectors if i % 2 else (i - 1) % sectors) for i in range(sectors)]
    near = swap(send, 1)
    far = lax.ppermute(shift, "azi", offset)
    axial_low, axial_high = across("ax", row_top, row_out, row_out)
    edge_low, edge_high = across("rad", column[0], column[-1], column[0])

    mixed = keep + near[: pairs * chunk]
    parts = [mixed[k * chunk : (k + 1) * chunk] for k in range(pairs)]
    arrived = [mixed]
    for k in range(1, pairs):
        arrived.append(swap(jnp.concatenate(parts[k:] + parts[:k], axis=0), 2 * k))
    summed = functools.reduce(
        jnp.add, [mixed] + [jnp.concatenate([x[(pairs - k) * chunk :], x[: (pairs - k) * chunk]], axis=0) for k, x in enumerate(arrived) if k]
    )

    before = pl.pallas_call(
        stencil,
        out_shape=struct(fields.shape, f32),
        in_specs=[VMEM] * 8,
        out_specs=VMEM,
        compiler_params=params(12),
        cost_estimate=cost(1 << 28, 1 << 23),
        name="stencil",
    )(fields, swirl_speed, ghost_mask, tiles, near, far, edge_low, edge_high)

    feed = pl.pallas_call(
        functools.partial(feed_rows, slots),
        out_shape=struct((cells * SUB + SUB, width), f32),
        in_specs=[SMEM] + [VMEM] * pairs,
        out_specs=VMEM,
        compiler_params=params(8),
        cost_estimate=cost(1 << 25, 1 << 20),
        name="feed",
    )(feed_target[0], *arrived)

    other = swap(summed, 1)

    return pl.pallas_call(
        functools.partial(finish, chunk, length),
        out_shape=struct(fields.shape, f32),
        in_specs=[VMEM] * 8,
        out_specs=HBM,
        scratch_shapes=[
            pltpu.VMEM((count * modes, width), f32),
            pltpu.VMEM((count, cells, width), f32),
            pltpu.VMEM(fields.shape, f32),
            pltpu.SemaphoreType.DMA((count, cells // SUB)),
        ],
        compiler_params=params(16),
        cost_estimate=cost(1 << 26, 1 << 23),
        name="finish",
    )(axial_low, axial_high, row_top, summed, other, weights, feed, before)


def solution(mesh):
    return jax.shard_map(
        body,
        mesh=mesh,
        in_specs=(
            P(None, "azi", "ax", "rad"),
            P("azi", "ax", "rad"),
            P("azi", "ax", "rad"),
            P("azi", "ax"),
            P(),
            P("azi", None, None),
            P("azi", None, None, "rad"),
            P("azi", None, None),
        ),
        out_specs=P(None, "azi", "ax", "rad"),
        check_vma=False,
    )
```

```python
import functools
import math

import jax
import jax.numpy as jnp
from jax import lax
from jax.experimental import pallas as pl
from jax.experimental.pallas import tpu as pltpu
from jax.sharding import PartitionSpec as P


TILE = 16
HEAD = 4
LANES = 128
UNROLL = 4
SUB = 8
HIGH = lax.Precision.HIGHEST
VMEM = pl.BlockSpec(memory_space=pltpu.VMEM)
SMEM = pl.BlockSpec(memory_space=pltpu.SMEM)
HBM = pl.BlockSpec(memory_space=pltpu.HBM)
f32 = jnp.float32


def params(mib):
    return pltpu.CompilerParams(vmem_limit_bytes=mib << 20)


def cost(flops, size):
    return pl.CostEstimate(flops=flops, bytes_accessed=size, transcendentals=0)


def in_hbm(x):
    return pltpu.with_memory_space_constraint(x, pltpu.HBM)


def phases(length, first_cell, cell_count, mode_count):
    cells = first_cell + jnp.arange(cell_count, dtype=jnp.int32)
    order = jnp.arange(1, mode_count + 1, dtype=jnp.int32)
    angle = (order[:, None] * cells[None, :] % length).astype(f32) * (2.0 * math.pi / length)
    turned = (cells[:, None] * order[None, :] % length).astype(f32) * (2.0 * math.pi / length)
    return (
        jnp.concatenate([jnp.cos(angle), jnp.sin(angle)], axis=0),
        jnp.concatenate([jnp.cos(turned), jnp.sin(turned)], axis=1),
    )


def prepare(
    chunk, fields, phase, rates, profile, keep, send, shift, row_top, row_out, column, local, rate, plenum, tile, sem
):
    azi, ax, rad = lax.axis_index("azi"), lax.axis_index("ax"), lax.axis_index("rad")
    last_ax = lax.axis_size("ax") - 1
    count, cells, depth, width = fields.shape
    sectors, slots, _ = profile.shape
    pairs = sectors // 2
    parity, place = azi % 2, azi // 2
    base = pairs * chunk
    t_pair = jnp.where(parity == 0, cells - 1, 0)
    t_shift = jnp.where(parity == 0, 0, cells - 1)
    row_sent = jnp.where((ax == 0) & (last_ax == 1), depth - 1, 0)
    if lax.axis_size("rad") == 2:
        more = jnp.where(rad == 0, 1, 0)
        sides = [(jnp.where(rad == 0, width - LANES, 0), lambda j: (j + more) if j < LANES - 1 else j * (1 - more))]
    else:
        sides = [(width - LANES, lambda j: (j + 1) % LANES), (0, lambda j: j)]
    first = pltpu.make_async_copy(fields.at[:, :, depth - 1, :], row_top, sem.at[0])
    first.start()
    copies = []
    for c in range(count):
        rows = slice(base + c * depth, base + (c + 1) * depth)
        copies.append(pltpu.make_async_copy(fields.at[c, t_pair], send.at[rows], sem.at[1 + 2 * c]))
        rows = slice(c * depth, (c + 1) * depth)
        copies.append(pltpu.make_async_copy(fields.at[c, t_shift], shift.at[rows], sem.at[2 + 2 * c]))
    edges = [
        pltpu.make_async_copy(
            fields.at[:, :, :, pl.ds(pl.multiple_of(side, LANES), LANES)], tile.at[e], sem.at[6 + 2 * count + e]
        )
        for e, (side, _) in enumerate(sides)
    ]
    for one in copies:
        one.start()
    for edge in edges:
        edge.start()
    face = pltpu.make_async_copy(fields.at[:, :, row_sent, :], row_out, sem.at[2 + 2 * count])
    face.start()
    supply = pltpu.make_async_copy(profile, plenum, sem.at[3 + 2 * count])
    supply.start()
    factor = pltpu.make_async_copy(rates, rate, sem.at[4 + 2 * count])
    factor.start()
    whole = pltpu.make_async_copy(fields, local, sem.at[5 + 2 * count])
    whole.start()

    @pl.when(ax == last_ax)
    def _():
        first.wait()
        supply.wait()
        factor.wait()
        sums = [
            jnp.dot(phase[...], row_top[c], precision=HIGH, preferred_element_type=f32)
            for c in range(count)
        ]
        modes = phase.shape[0]
        length = count * modes // sectors
        blocks = []
        for s in range(sectors):
            c, m = divmod(s * length, modes)
            blocks.append(sums[c][m : m + length])
        for q in range(pairs):
            even, odd = blocks[2 * q], blocks[2 * q + 1]
            at = q * chunk
            keep[at : at + length] = jnp.where(parity == 0, even, odd)
            send[at : at + length] = jnp.where(parity == 0, odd, even)
            if chunk > length:
                keep[at + length : at + chunk] = jnp.zeros((chunk - length, width), f32)
                send[at + length : at + chunk] = jnp.zeros((chunk - length, width), f32)

    @pl.when(ax != last_ax)
    def _():
        first.wait()
        supply.wait()
        factor.wait()
        turned = rate[...].T
        for q in range(pairs):
            at = pl.multiple_of((q ^ place) * chunk, SUB)
            even = turned[:, 2 * q : 2 * q + 1] * plenum[2 * q]
            odd = turned[:, 2 * q + 1 : 2 * q + 2] * plenum[2 * q + 1]
            own = jnp.where(parity == 0, even, odd)
            other = jnp.where(parity == 0, odd, even)
            for p in range(2):
                rows = pl.ds(pl.multiple_of(at + p * slots, SUB), slots)
                keep[rows] = jnp.where(parity == p, own, 0.0)
                send[rows] = jnp.where(parity == p, other, 0.0)
            if chunk > 2 * slots:
                rest = pl.ds(pl.multiple_of(at + 2 * slots, SUB), chunk - 2 * slots)
                keep[rest] = jnp.zeros((chunk - 2 * slots, width), f32)
                send[rest] = jnp.zeros((chunk - 2 * slots, width), f32)

    lane = lax.broadcasted_iota(jnp.int32, (SUB, LANES), 1)
    halves = depth // SUB
    for e, (_, by) in enumerate(sides):
        edges[e].wait()
        for g in range(column.shape[1]):
            acc = jnp.zeros((SUB, LANES), f32)
            for j in range(LANES):
                c, rest = divmod(g * LANES + j, cells * halves)
                t, h = divmod(rest, halves)
                piece = tile[e, c, t, h * SUB : (h + 1) * SUB, :]
                acc = jnp.where(lane == j, pltpu.roll(piece, by(j), 1), acc)
            column[e, g] = acc
    for one in copies:
        one.wait()
    face.wait()
    whole.wait()


def stencil(fields, swirl, mask, flags, near, shift, column_low, column_high, out):
    azi, rad = lax.axis_index("azi"), lax.axis_index("rad")
    last_rad = lax.axis_size("rad") - 1
    count, cells, depth, width = fields.shape
    base = near.shape[0] - count * depth
    parity = azi % 2
    halves = depth // SUB
    blocks = width // LANES
    lane = lax.broadcasted_iota(jnp.int32, (SUB, LANES), 1)
    row = lax.broadcasted_iota(jnp.int32, (SUB, LANES), 0)
    at_left, at_right = lane == 0, lane == LANES - 1
    at_low, at_high = row == 0, row == SUB - 1
    has_left, has_right = rad > 0, rad < last_rad
    turned = (0.5 * flags[...].astype(f32)).T

    def cut(h, l):
        return slice(h * SUB, (h + 1) * SUB), slice(l * LANES, (l + 1) * LANES)

    def slab(t, tile, before, after):
        levels = [jnp.broadcast_to(tile[h], (SUB, LANES)) for h in range(halves)]
        for c in range(count):
            edges = []
            for h in range(halves):
                n = (c * cells + t) * halves + h
                g, j = n // LANES, n % LANES
                edges.append((
                    jnp.where(has_left, pltpu.roll(column_low[g], (LANES - j) % LANES, 1), 0.0),
                    jnp.where(has_right, pltpu.roll(column_high[g], LANES - 1 - j, 1), 0.0),
                ))
            parts = [[fields[(c, t) + cut(h, l)] for l in range(blocks)] for h in range(halves)]
            ups = [[pltpu.roll(v, 1, 1) for v in p] for p in parts]
            downs = [[pltpu.roll(v, LANES - 1, 1) for v in p] for p in parts]
            for l in range(blocks):
                lows = [pltpu.roll(parts[h][l], 1, 0) for h in range(halves)]
                highs = [pltpu.roll(parts[h][l], SUB - 1, 0) for h in range(halves)]
                for h in range(halves):
                    left = jnp.where(at_left, ups[h][l - 1] if l else edges[h][0], ups[h][l])
                    right = jnp.where(at_right, downs[h][l + 1] if l + 1 < blocks else edges[h][1], downs[h][l])
                    low = jnp.where(at_low, lows[h - 1] if h else 0.0, lows[h])
                    high = jnp.where(at_high, highs[h + 1] if h + 1 < halves else 0.0, highs[h])
                    total = (left + right) + (low + high) + after(c, h, l)
                    speed = swirl[(t,) + cut(h, l)]
                    value = parts[h][l] * (0.4 - speed) + before(c, h, l) * (speed + 0.1) + 0.1 * total
                    if c == 0:
                        out[(0, t) + cut(h, l)] = value
                    else:
                        live = jnp.where(mask[(t,) + cut(h, l)] == 0, levels[h], 0.0) * parts[h][l]
                        energy = fields[(0, t) + cut(h, l)]
                        burn = live + live * jnp.tanh(2.0 * energy - 1.0)
                        out[(0, t) + cut(h, l)] += burn
                        out[(1, t) + cut(h, l)] = value - 0.5 * burn

    def halo(use_near):
        def value(c, h, l):
            _, lanes = cut(h, l)
            a = near[base + c * depth + h * SUB : base + c * depth + (h + 1) * SUB, lanes]
            b = shift[c * depth + h * SUB : c * depth + (h + 1) * SUB, lanes]
            return jnp.where(use_near, a, b)

        return value

    def inside(t):
        return lambda c, h, l: fields[(c, t) + cut(h, l)]

    tiles = [[turned[h * SUB : (h + 1) * SUB, k : k + 1] for h in range(halves)] for k in range(cells // TILE)]
    for k in range(cells // TILE):
        first, last = k * TILE, (k + 1) * TILE
        if first == 0:
            slab(0, tiles[k], halo(parity == 1), inside(1))
            first = 1
        if last == cells:
            last = cells - 1

        def step(t, carry, tile=tiles[k]):
            slab(t, tile, inside(t - 1), inside(t + 1))
            return carry

        lax.fori_loop(first, last, step, 0, unroll=UNROLL)

        if last == cells - 1:
            slab(cells - 1, tiles[k], inside(cells - 2), halo(parity == 0))


def feed_rows(slots, targets, *refs):
    *arrived, feed = refs
    place = lax.axis_index("azi") // 2
    rows = feed.shape[0] - SUB
    feed[...] = jnp.zeros(feed.shape, f32)

    @pl.when(lax.axis_index("ax") == 0)
    def _():
        for k, block in enumerate(arrived):
            for p in range(2):
                for j in range(slots):
                    target = targets[2 * (place ^ k) + p, j]
                    at = jnp.where(target >= 0, target // HEAD * SUB + target % HEAD, rows)
                    r = p * slots + j
                    feed[pl.ds(at, 1), :] += block[r : r + 1, :]


def finish(chunk, length, axial_low, axial_high, row_top, own, other, weights, feed, before, out, modes, high, result, sem):
    azi, ax = lax.axis_index("azi"), lax.axis_index("ax")
    last_ax = lax.axis_size("ax") - 1
    count, cells, depth, width = before.shape
    parity = azi % 2
    pairs = own.shape[0] // chunk

    @pl.when(ax == last_ax)
    def _():
        for k in range(pairs):
            for ref, p in ((own, parity), (other, 1 - parity)):
                at = pl.multiple_of((2 * k + p) * length, SUB)
                modes[pl.ds(at, length)] = ref[k * chunk : k * chunk + length]
        per = modes.shape[0] // count
        for c in range(count):
            rebuilt = jnp.dot(
                weights[c], modes[c * per : (c + 1) * per], precision=HIGH, preferred_element_type=f32
            )
            high[c] = 0.1 * row_top[c] - rebuilt

    @pl.when(ax != last_ax)
    def _():
        for c in range(count):
            high[c] = 0.1 * axial_high[c]

    scale = jnp.where(ax > 0, 0.1, 0.0)
    row = lax.broadcasted_iota(jnp.int32, (SUB, width), 0)
    group = SUB
    copies = []
    for b in range(cells // group):
        for c in range(count):
            low_rows = scale * axial_low[c, b * group : (b + 1) * group]
            high_rows = high[c, b * group : (b + 1) * group]
            for i in range(group):
                t = b * group + i
                head = before[c, t, :SUB] + jnp.where(row == 0, low_rows[i : i + 1], 0.0)
                if c == 1:
                    head = head + feed[t * SUB : (t + 1) * SUB]
                result[c, t, :SUB] = head
                if depth > 2 * SUB:
                    result[c, t, SUB : depth - SUB] = before[c, t, SUB : depth - SUB]
                tail = before[c, t, depth - SUB :]
                result[c, t, depth - SUB :] = tail + jnp.where(row == SUB - 1, high_rows[i : i + 1], 0.0)
            cells_at = pl.ds(b * group, group)
            copy = pltpu.make_async_copy(result.at[c, cells_at], out.at[c, cells_at], sem.at[c, b])
            copy.start()
            copies.append(copy)
    for copy in copies:
        copy.wait()


def body(fields, swirl_speed, ghost_mask, tile_flags, outlet_gain, feed_rate, plenum, feed_target):
    sectors, radials = lax.axis_size("azi"), lax.axis_size("rad")
    count, cells, depth, width = fields.shape
    half_modes = outlet_gain.shape[1]
    modes = 2 * half_modes
    slots = plenum.shape[2]
    length = count * modes // sectors
    chunk = max(length, 2 * slots)
    pairs = sectors // 2
    total_cells = cells * sectors
    phase, phase_t = phases(total_cells, lax.axis_index("azi") * cells, cells, half_modes)
    gain = jnp.concatenate([outlet_gain, outlet_gain], axis=1)
    weights = phase_t[None] * gain[:, None, :] * (0.1 * 2.0 / math.sqrt(half_modes * total_cells))
    groups = count * cells * depth // SUB // LANES

    struct = jax.ShapeDtypeStruct
    keep, send, shift, row_top, row_out, column, local = pl.pallas_call(
        functools.partial(prepare, chunk),
        out_shape=(
            struct((pairs * chunk, width), f32),
            struct((pairs * chunk + count * depth, width), f32),
            struct((count * depth, width), f32),
            struct((count, cells, width), f32),
            struct((count, cells, width), f32),
            struct((1 if radials == 2 else 2, groups, SUB, LANES), f32),
            struct(fields.shape, f32),
        ),
        in_specs=[HBM, VMEM, HBM, HBM],
        out_specs=[VMEM] * 7,
        scratch_shapes=[
            pltpu.VMEM((sectors, slots), f32),
            pltpu.VMEM((sectors, slots, width), f32),
            pltpu.VMEM((1 if radials == 2 else 2, count, cells, depth, LANES), f32),
            pltpu.SemaphoreType.DMA((2 * count + 8,)),
        ],
        compiler_params=params(12),
        cost_estimate=cost(1 << 26, 1 << 21),
        name="prepare",
    )(in_hbm(fields), phase, in_hbm(feed_rate[0]), in_hbm(plenum[0]))

    def swap(x, k):
        return lax.ppermute(x, "azi", [(i, i ^ k) for i in range(sectors)])

    def across(axis, to_high, to_low, to_only):
        size = lax.axis_size(axis)
        if size == 2:
            received = lax.ppermute(to_only, axis, [(0, 1), (1, 0)])
            return received, received
        ups = [(i, i + 1) for i in range(size - 1)]
        return lax.ppermute(to_high, axis, ups), lax.ppermute(to_low, axis, [(b, a) for a, b in ups])

    offset = [(i, (i + 1) % sectors if i % 2 else (i - 1) % sectors) for i in range(sectors)]
    near = swap(send, 1)
    far = lax.ppermute(shift, "azi", offset)
    axial_low, axial_high = across("ax", row_top, row_out, row_out)
    edge_low, edge_high = across("rad", column[0], column[-1], column[0])

    mixed = keep + near[: pairs * chunk]
    parts = [mixed[k * chunk : (k + 1) * chunk] for k in range(pairs)]
    arrived = [mixed]
    for k in range(1, pairs):
        arrived.append(swap(jnp.concatenate(parts[k:] + parts[:k], axis=0), 2 * k))
    summed = functools.reduce(
        jnp.add, [mixed] + [jnp.concatenate([x[(pairs - k) * chunk :], x[: (pairs - k) * chunk]], axis=0) for k, x in enumerate(arrived) if k]
    )

    before = pl.pallas_call(
        stencil,
        out_shape=struct(fields.shape, f32),
        in_specs=[VMEM] * 8,
        out_specs=VMEM,
        compiler_params=params(12),
        cost_estimate=cost(1 << 28, 1 << 23),
        name="stencil",
    )(local, swirl_speed, ghost_mask, tile_flags, near, far, edge_low, edge_high)

    feed = pl.pallas_call(
        functools.partial(feed_rows, slots),
        out_shape=struct((cells * SUB + SUB, width), f32),
        in_specs=[SMEM] + [VMEM] * pairs,
        out_specs=VMEM,
        compiler_params=params(8),
        cost_estimate=cost(1 << 25, 1 << 20),
        name="feed",
    )(feed_target[0], *arrived)

    other = swap(summed, 1)

    return pl.pallas_call(
        functools.partial(finish, chunk, length),
        out_shape=struct(fields.shape, f32),
        in_specs=[VMEM] * 8,
        out_specs=HBM,
        scratch_shapes=[
            pltpu.VMEM((count * modes, width), f32),
            pltpu.VMEM((count, cells, width), f32),
            pltpu.VMEM(fields.shape, f32),
            pltpu.SemaphoreType.DMA((count, cells // SUB)),
        ],
        compiler_params=params(16),
        cost_estimate=cost(1 << 26, 1 << 23),
        name="finish",
    )(axial_low, axial_high, row_top, summed, other, weights, feed, before)


def solution(mesh):
    return jax.shard_map(
        body,
        mesh=mesh,
        in_specs=(
            P(None, "azi", "ax", "rad"),
            P("azi", "ax", "rad"),
            P("azi", "ax", "rad"),
            P("azi", "ax"),
            P(),
            P("azi", None, None),
            P("azi", None, None, "rad"),
            P("azi", None, None),
        ),
        out_specs=P(None, "azi", "ax", "rad"),
        check_vma=False,
    )
```

```python
import functools
import math

import jax
import jax.numpy as jnp
from jax import lax
from jax.experimental import pallas as pl
from jax.experimental.pallas import tpu as pltpu
from jax.sharding import PartitionSpec as P


TILE = 16
HEAD = 4
LANES = 128
UNROLL = 4
SUB = 8
HIGH = lax.Precision.HIGHEST
VMEM = pl.BlockSpec(memory_space=pltpu.VMEM)
SMEM = pl.BlockSpec(memory_space=pltpu.SMEM)
HBM = pl.BlockSpec(memory_space=pltpu.HBM)
f32 = jnp.float32


def params(mib):
    return pltpu.CompilerParams(vmem_limit_bytes=mib << 20)


def cost(flops, size):
    return pl.CostEstimate(flops=flops, bytes_accessed=size, transcendentals=0)


def in_hbm(x):
    return pltpu.with_memory_space_constraint(x, pltpu.HBM)


def phases(length, first_cell, cell_count, mode_count):
    cells = first_cell + jnp.arange(cell_count, dtype=jnp.int32)
    order = jnp.arange(1, mode_count + 1, dtype=jnp.int32)
    angle = (order[:, None] * cells[None, :] % length).astype(f32) * (2.0 * math.pi / length)
    turned = (cells[:, None] * order[None, :] % length).astype(f32) * (2.0 * math.pi / length)
    return (
        jnp.concatenate([jnp.cos(angle), jnp.sin(angle)], axis=0),
        jnp.concatenate([jnp.cos(turned), jnp.sin(turned)], axis=1),
    )


def prepare(
    chunk, fields, phase, rates, profile, keep, send, shift, row_top, row_out, column, rate, plenum, tile, sem
):
    azi, ax, rad = lax.axis_index("azi"), lax.axis_index("ax"), lax.axis_index("rad")
    last_ax = lax.axis_size("ax") - 1
    count, cells, depth, width = fields.shape
    sectors, slots, _ = profile.shape
    pairs = sectors // 2
    parity, place = azi % 2, azi // 2
    base = pairs * chunk
    t_pair = jnp.where(parity == 0, cells - 1, 0)
    t_shift = jnp.where(parity == 0, 0, cells - 1)
    row_sent = jnp.where((ax == 0) & (last_ax == 1), depth - 1, 0)
    if lax.axis_size("rad") == 2:
        more = jnp.where(rad == 0, 1, 0)
        sides = [(jnp.where(rad == 0, width - LANES, 0), lambda j: (j + more) if j < LANES - 1 else j * (1 - more))]
    else:
        sides = [(width - LANES, lambda j: (j + 1) % LANES), (0, lambda j: j)]
    first = pltpu.make_async_copy(fields.at[:, :, depth - 1, :], row_top, sem.at[0])
    first.start()
    copies = []
    for c in range(count):
        rows = slice(base + c * depth, base + (c + 1) * depth)
        copies.append(pltpu.make_async_copy(fields.at[c, t_pair], send.at[rows], sem.at[1 + 2 * c]))
        rows = slice(c * depth, (c + 1) * depth)
        copies.append(pltpu.make_async_copy(fields.at[c, t_shift], shift.at[rows], sem.at[2 + 2 * c]))
    edges = [
        pltpu.make_async_copy(
            fields.at[:, :, :, pl.ds(pl.multiple_of(side, LANES), LANES)], tile.at[e], sem.at[5 + 2 * count + e]
        )
        for e, (side, _) in enumerate(sides)
    ]
    for one in copies:
        one.start()
    for edge in edges:
        edge.start()
    face = pltpu.make_async_copy(fields.at[:, :, row_sent, :], row_out, sem.at[2 + 2 * count])
    face.start()
    supply = pltpu.make_async_copy(profile, plenum, sem.at[3 + 2 * count])
    supply.start()
    factor = pltpu.make_async_copy(rates, rate, sem.at[4 + 2 * count])
    factor.start()

    @pl.when(ax == last_ax)
    def _():
        first.wait()
        supply.wait()
        factor.wait()
        sums = [
            jnp.dot(phase[...], row_top[c], precision=HIGH, preferred_element_type=f32)
            for c in range(count)
        ]
        modes = phase.shape[0]
        length = count * modes // sectors
        blocks = []
        for s in range(sectors):
            c, m = divmod(s * length, modes)
            blocks.append(sums[c][m : m + length])
        for q in range(pairs):
            even, odd = blocks[2 * q], blocks[2 * q + 1]
            at = q * chunk
            keep[at : at + length] = jnp.where(parity == 0, even, odd)
            send[at : at + length] = jnp.where(parity == 0, odd, even)
            if chunk > length:
                keep[at + length : at + chunk] = jnp.zeros((chunk - length, width), f32)
                send[at + length : at + chunk] = jnp.zeros((chunk - length, width), f32)

    @pl.when(ax != last_ax)
    def _():
        first.wait()
        supply.wait()
        factor.wait()
        turned = rate[...].T
        for q in range(pairs):
            at = pl.multiple_of((q ^ place) * chunk, SUB)
            even = turned[:, 2 * q : 2 * q + 1] * plenum[2 * q]
            odd = turned[:, 2 * q + 1 : 2 * q + 2] * plenum[2 * q + 1]
            own = jnp.where(parity == 0, even, odd)
            other = jnp.where(parity == 0, odd, even)
            for p in range(2):
                rows = pl.ds(pl.multiple_of(at + p * slots, SUB), slots)
                keep[rows] = jnp.where(parity == p, own, 0.0)
                send[rows] = jnp.where(parity == p, other, 0.0)
            if chunk > 2 * slots:
                rest = pl.ds(pl.multiple_of(at + 2 * slots, SUB), chunk - 2 * slots)
                keep[rest] = jnp.zeros((chunk - 2 * slots, width), f32)
                send[rest] = jnp.zeros((chunk - 2 * slots, width), f32)

    lane = lax.broadcasted_iota(jnp.int32, (SUB, LANES), 1)
    halves = depth // SUB
    for e, (_, by) in enumerate(sides):
        edges[e].wait()
        for g in range(column.shape[1]):
            acc = jnp.zeros((SUB, LANES), f32)
            for j in range(LANES):
                c, rest = divmod(g * LANES + j, cells * halves)
                t, h = divmod(rest, halves)
                piece = tile[e, c, t, h * SUB : (h + 1) * SUB, :]
                acc = jnp.where(lane == j, pltpu.roll(piece, by(j), 1), acc)
            column[e, g] = acc
    for one in copies:
        one.wait()
    face.wait()


def stencil(source, swirl, mask, flags, near, shift, column_low, column_high, out, fields, levels, sem):
    azi, rad = lax.axis_index("azi"), lax.axis_index("rad")
    last_rad = lax.axis_size("rad") - 1
    count, cells, depth, width = fields.shape
    base = near.shape[0] - count * depth
    parity = azi % 2
    halves = depth // SUB
    blocks = width // LANES
    lane = lax.broadcasted_iota(jnp.int32, (SUB, LANES), 1)
    row = lax.broadcasted_iota(jnp.int32, (SUB, LANES), 0)
    at_left, at_right = lane == 0, lane == LANES - 1
    at_low, at_high = row == 0, row == SUB - 1
    has_left, has_right = rad > 0, rad < last_rad
    pieces = [slice(k * TILE, (k + 1) * TILE) for k in range(cells // TILE)]
    copies = [pltpu.make_async_copy(source.at[:, p], fields.at[:, p], sem.at[k]) for k, p in enumerate(pieces)]
    for copy in copies:
        copy.start()
    turned = (0.5 * flags[...].astype(f32)).T
    for k in range(cells // TILE):
        levels[k] = jnp.broadcast_to(turned[:, k : k + 1], (depth, LANES))

    def cut(h, l):
        return slice(h * SUB, (h + 1) * SUB), slice(l * LANES, (l + 1) * LANES)

    def slab(t, before, after):
        level = levels[t // TILE]
        for c in range(count):
            edges = []
            for h in range(halves):
                n = (c * cells + t) * halves + h
                g, j = n // LANES, n % LANES
                edges.append((
                    jnp.where(has_left, pltpu.roll(column_low[g], (LANES - j) % LANES, 1), 0.0),
                    jnp.where(has_right, pltpu.roll(column_high[g], LANES - 1 - j, 1), 0.0),
                ))
            parts = [[fields[(c, t) + cut(h, l)] for l in range(blocks)] for h in range(halves)]
            ups = [[pltpu.roll(v, 1, 1) for v in p] for p in parts]
            downs = [[pltpu.roll(v, LANES - 1, 1) for v in p] for p in parts]
            for l in range(blocks):
                lows = [pltpu.roll(parts[h][l], 1, 0) for h in range(halves)]
                highs = [pltpu.roll(parts[h][l], SUB - 1, 0) for h in range(halves)]
                for h in range(halves):
                    left = jnp.where(at_left, ups[h][l - 1] if l else edges[h][0], ups[h][l])
                    right = jnp.where(at_right, downs[h][l + 1] if l + 1 < blocks else edges[h][1], downs[h][l])
                    low = jnp.where(at_low, lows[h - 1] if h else 0.0, lows[h])
                    high = jnp.where(at_high, highs[h + 1] if h + 1 < halves else 0.0, highs[h])
                    total = (left + right) + (low + high) + after(c, h, l)
                    speed = swirl[(t,) + cut(h, l)]
                    value = parts[h][l] * (0.4 - speed) + before(c, h, l) * (speed + 0.1) + 0.1 * total
                    if c == 0:
                        out[(0, t) + cut(h, l)] = value
                    else:
                        live = jnp.where(mask[(t,) + cut(h, l)] == 0, level[h * SUB : (h + 1) * SUB], 0.0) * parts[h][l]
                        energy = fields[(0, t) + cut(h, l)]
                        burn = live + live * jnp.tanh(2.0 * energy - 1.0)
                        out[(0, t) + cut(h, l)] += burn
                        out[(1, t) + cut(h, l)] = value - 0.5 * burn

    def halo(use_near):
        def value(c, h, l):
            _, lanes = cut(h, l)
            a = near[base + c * depth + h * SUB : base + c * depth + (h + 1) * SUB, lanes]
            b = shift[c * depth + h * SUB : c * depth + (h + 1) * SUB, lanes]
            return jnp.where(use_near, a, b)

        return value

    def inside(t):
        return lambda c, h, l: fields[(c, t) + cut(h, l)]

    def step(t, carry):
        slab(t, inside(t - 1), inside(t + 1))
        return carry

    copies[0].wait()
    slab(0, halo(parity == 1), inside(1))
    for k, copy in enumerate(copies):
        if k:
            copy.wait()
        lax.fori_loop(k * TILE - 1 if k else 1, (k + 1) * TILE - 1, step, 0, unroll=UNROLL)
    slab(cells - 1, inside(cells - 2), halo(parity == 0))


def feed_rows(slots, targets, *refs):
    *arrived, feed = refs
    place = lax.axis_index("azi") // 2
    rows = feed.shape[0] - SUB
    feed[...] = jnp.zeros(feed.shape, f32)

    @pl.when(lax.axis_index("ax") == 0)
    def _():
        for k, block in enumerate(arrived):
            for p in range(2):
                for j in range(slots):
                    target = targets[2 * (place ^ k) + p, j]
                    at = jnp.where(target >= 0, target // HEAD * SUB + target % HEAD, rows)
                    r = p * slots + j
                    feed[pl.ds(at, 1), :] += block[r : r + 1, :]


def finish(chunk, length, axial_low, axial_high, row_top, own, other, weights, feed, before, out, modes, high, result, sem):
    azi, ax = lax.axis_index("azi"), lax.axis_index("ax")
    last_ax = lax.axis_size("ax") - 1
    count, cells, depth, width = before.shape
    parity = azi % 2
    pairs = own.shape[0] // chunk

    @pl.when(ax == last_ax)
    def _():
        for k in range(pairs):
            for ref, p in ((own, parity), (other, 1 - parity)):
                at = pl.multiple_of((2 * k + p) * length, SUB)
                modes[pl.ds(at, length)] = ref[k * chunk : k * chunk + length]
        per = modes.shape[0] // count
        for c in range(count):
            rebuilt = jnp.dot(
                weights[c], modes[c * per : (c + 1) * per], precision=HIGH, preferred_element_type=f32
            )
            high[c] = 0.1 * row_top[c] - rebuilt

    @pl.when(ax != last_ax)
    def _():
        for c in range(count):
            high[c] = 0.1 * axial_high[c]

    scale = jnp.where(ax > 0, 0.1, 0.0)
    row = lax.broadcasted_iota(jnp.int32, (SUB, width), 0)
    group = SUB
    copies = []
    for b in range(cells // group):
        for c in range(count):
            low_rows = scale * axial_low[c, b * group : (b + 1) * group]
            high_rows = high[c, b * group : (b + 1) * group]
            for i in range(group):
                t = b * group + i
                head = before[c, t, :SUB] + jnp.where(row == 0, low_rows[i : i + 1], 0.0)
                if c == 1:
                    head = head + feed[t * SUB : (t + 1) * SUB]
                result[c, t, :SUB] = head
                if depth > 2 * SUB:
                    result[c, t, SUB : depth - SUB] = before[c, t, SUB : depth - SUB]
                tail = before[c, t, depth - SUB :]
                result[c, t, depth - SUB :] = tail + jnp.where(row == SUB - 1, high_rows[i : i + 1], 0.0)
            cells_at = pl.ds(b * group, group)
            copy = pltpu.make_async_copy(result.at[c, cells_at], out.at[c, cells_at], sem.at[c, b])
            copy.start()
            copies.append(copy)
    for copy in copies:
        copy.wait()


def body(fields, swirl_speed, ghost_mask, tile_flags, outlet_gain, feed_rate, plenum, feed_target):
    sectors, radials = lax.axis_size("azi"), lax.axis_size("rad")
    count, cells, depth, width = fields.shape
    half_modes = outlet_gain.shape[1]
    modes = 2 * half_modes
    slots = plenum.shape[2]
    length = count * modes // sectors
    chunk = max(length, 2 * slots)
    pairs = sectors // 2
    total_cells = cells * sectors
    phase, phase_t = phases(total_cells, lax.axis_index("azi") * cells, cells, half_modes)
    gain = jnp.concatenate([outlet_gain, outlet_gain], axis=1)
    weights = phase_t[None] * gain[:, None, :] * (0.1 * 2.0 / math.sqrt(half_modes * total_cells))
    groups = count * cells * depth // SUB // LANES

    struct = jax.ShapeDtypeStruct
    keep, send, shift, row_top, row_out, column = pl.pallas_call(
        functools.partial(prepare, chunk),
        out_shape=(
            struct((pairs * chunk, width), f32),
            struct((pairs * chunk + count * depth, width), f32),
            struct((count * depth, width), f32),
            struct((count, cells, width), f32),
            struct((count, cells, width), f32),
            struct((1 if radials == 2 else 2, groups, SUB, LANES), f32),
        ),
        in_specs=[HBM, VMEM, HBM, HBM],
        out_specs=[VMEM] * 6,
        scratch_shapes=[
            pltpu.VMEM((sectors, slots), f32),
            pltpu.VMEM((sectors, slots, width), f32),
            pltpu.VMEM((1 if radials == 2 else 2, count, cells, depth, LANES), f32),
            pltpu.SemaphoreType.DMA((2 * count + 7,)),
        ],
        compiler_params=params(12),
        cost_estimate=cost(1 << 26, 1 << 21),
        name="prepare",
    )(in_hbm(fields), phase, in_hbm(feed_rate[0]), in_hbm(plenum[0]))

    def swap(x, k):
        return lax.ppermute(x, "azi", [(i, i ^ k) for i in range(sectors)])

    def across(axis, to_high, to_low, to_only):
        size = lax.axis_size(axis)
        if size == 2:
            received = lax.ppermute(to_only, axis, [(0, 1), (1, 0)])
            return received, received
        ups = [(i, i + 1) for i in range(size - 1)]
        return lax.ppermute(to_high, axis, ups), lax.ppermute(to_low, axis, [(b, a) for a, b in ups])

    offset = [(i, (i + 1) % sectors if i % 2 else (i - 1) % sectors) for i in range(sectors)]
    near = swap(send, 1)
    far = lax.ppermute(shift, "azi", offset)
    axial_low, axial_high = across("ax", row_top, row_out, row_out)
    edge_low, edge_high = across("rad", column[0], column[-1], column[0])

    mixed = keep + near[: pairs * chunk]
    parts = [mixed[k * chunk : (k + 1) * chunk] for k in range(pairs)]
    arrived = [mixed]
    for k in range(1, pairs):
        arrived.append(swap(jnp.concatenate(parts[k:] + parts[:k], axis=0), 2 * k))
    summed = functools.reduce(
        jnp.add, [mixed] + [jnp.concatenate([x[(pairs - k) * chunk :], x[: (pairs - k) * chunk]], axis=0) for k, x in enumerate(arrived) if k]
    )

    before = pl.pallas_call(
        stencil,
        out_shape=struct(fields.shape, f32),
        in_specs=[HBM] + [VMEM] * 7,
        out_specs=VMEM,
        scratch_shapes=[
            pltpu.VMEM(fields.shape, f32),
            pltpu.VMEM((cells // TILE, depth, LANES), f32),
            pltpu.SemaphoreType.DMA((cells // TILE,)),
        ],
        compiler_params=params(12),
        cost_estimate=cost(1 << 28, 1 << 23),
        name="stencil",
    )(in_hbm(fields), swirl_speed, ghost_mask, tile_flags, near, far, edge_low, edge_high)

    feed = pl.pallas_call(
        functools.partial(feed_rows, slots),
        out_shape=struct((cells * SUB + SUB, width), f32),
        in_specs=[SMEM] + [VMEM] * pairs,
        out_specs=VMEM,
        compiler_params=params(8),
        cost_estimate=cost(1 << 25, 1 << 20),
        name="feed",
    )(feed_target[0], *arrived)

    other = swap(summed, 1)

    return pl.pallas_call(
        functools.partial(finish, chunk, length),
        out_shape=struct(fields.shape, f32),
        in_specs=[VMEM] * 8,
        out_specs=HBM,
        scratch_shapes=[
            pltpu.VMEM((count * modes, width), f32),
            pltpu.VMEM((count, cells, width), f32),
            pltpu.VMEM(fields.shape, f32),
            pltpu.SemaphoreType.DMA((count, cells // SUB)),
        ],
        compiler_params=params(16),
        cost_estimate=cost(1 << 26, 1 << 23),
        name="finish",
    )(axial_low, axial_high, row_top, summed, other, weights, feed, before)


def solution(mesh):
    return jax.shard_map(
        body,
        mesh=mesh,
        in_specs=(
            P(None, "azi", "ax", "rad"),
            P("azi", "ax", "rad"),
            P("azi", "ax", "rad"),
            P("azi", "ax"),
            P(),
            P("azi", None, None),
            P("azi", None, None, "rad"),
            P("azi", None, None),
        ),
        out_specs=P(None, "azi", "ax", "rad"),
        check_vma=False,
    )
```

```python
import functools
import math

import jax
import jax.numpy as jnp
from jax import lax
from jax.experimental import pallas as pl
from jax.experimental.pallas import tpu as pltpu
from jax.sharding import PartitionSpec as P


TILE = 16
HEAD = 4
LANES = 128
UNROLL = 4
SUB = 8
HIGH = lax.Precision.HIGHEST
VMEM = pl.BlockSpec(memory_space=pltpu.VMEM)
SMEM = pl.BlockSpec(memory_space=pltpu.SMEM)
HBM = pl.BlockSpec(memory_space=pltpu.HBM)
f32 = jnp.float32


def params(mib):
    return pltpu.CompilerParams(vmem_limit_bytes=mib << 20)


def cost(flops, size):
    return pl.CostEstimate(flops=flops, bytes_accessed=size, transcendentals=0)


def in_hbm(x):
    return pltpu.with_memory_space_constraint(x, pltpu.HBM)


def phases(length, first_cell, cell_count, mode_count):
    cells = first_cell + jnp.arange(cell_count, dtype=jnp.int32)
    order = jnp.arange(1, mode_count + 1, dtype=jnp.int32)
    angle = (order[:, None] * cells[None, :] % length).astype(f32) * (2.0 * math.pi / length)
    turned = (cells[:, None] * order[None, :] % length).astype(f32) * (2.0 * math.pi / length)
    return (
        jnp.concatenate([jnp.cos(angle), jnp.sin(angle)], axis=0),
        jnp.concatenate([jnp.cos(turned), jnp.sin(turned)], axis=1),
    )


def prepare(
    chunk, fields, phase, rates, profile, keep, send, shift, row_top, row_out, column, rate, plenum, tile, sem
):
    azi, ax, rad = lax.axis_index("azi"), lax.axis_index("ax"), lax.axis_index("rad")
    last_ax = lax.axis_size("ax") - 1
    count, cells, depth, width = fields.shape
    sectors, slots, _ = profile.shape
    pairs = sectors // 2
    parity, place = azi % 2, azi // 2
    base = pairs * chunk
    t_pair = jnp.where(parity == 0, cells - 1, 0)
    t_shift = jnp.where(parity == 0, 0, cells - 1)
    row_sent = jnp.where((ax == 0) & (last_ax == 1), depth - 1, 0)
    if lax.axis_size("rad") == 2:
        more = jnp.where(rad == 0, 1, 0)
        sides = [(jnp.where(rad == 0, width - LANES, 0), lambda j: (j + more) if j < LANES - 1 else j * (1 - more))]
    else:
        sides = [(width - LANES, lambda j: (j + 1) % LANES), (0, lambda j: j)]
    first = pltpu.make_async_copy(fields.at[:, :, depth - 1, :], row_top, sem.at[0])
    first.start()
    copies = []
    for c in range(count):
        rows = slice(base + c * depth, base + (c + 1) * depth)
        copies.append(pltpu.make_async_copy(fields.at[c, t_pair], send.at[rows], sem.at[1 + 2 * c]))
        rows = slice(c * depth, (c + 1) * depth)
        copies.append(pltpu.make_async_copy(fields.at[c, t_shift], shift.at[rows], sem.at[2 + 2 * c]))
    edges = [
        pltpu.make_async_copy(
            fields.at[:, :, :, pl.ds(pl.multiple_of(side, LANES), LANES)], tile.at[e], sem.at[5 + 2 * count + e]
        )
        for e, (side, _) in enumerate(sides)
    ]
    for one in copies:
        one.start()
    for edge in edges:
        edge.start()
    face = pltpu.make_async_copy(fields.at[:, :, row_sent, :], row_out, sem.at[2 + 2 * count])
    face.start()
    supply = pltpu.make_async_copy(profile, plenum, sem.at[3 + 2 * count])
    supply.start()
    factor = pltpu.make_async_copy(rates, rate, sem.at[4 + 2 * count])
    factor.start()

    @pl.when(ax == last_ax)
    def _():
        first.wait()
        supply.wait()
        factor.wait()
        sums = [
            jnp.dot(phase[...], row_top[c], precision=HIGH, preferred_element_type=f32)
            for c in range(count)
        ]
        modes = phase.shape[0]
        length = count * modes // sectors
        blocks = []
        for s in range(sectors):
            c, m = divmod(s * length, modes)
            blocks.append(sums[c][m : m + length])
        for q in range(pairs):
            even, odd = blocks[2 * q], blocks[2 * q + 1]
            at = q * chunk
            keep[at : at + length] = jnp.where(parity == 0, even, odd)
            send[at : at + length] = jnp.where(parity == 0, odd, even)
            if chunk > length:
                keep[at + length : at + chunk] = jnp.zeros((chunk - length, width), f32)
                send[at + length : at + chunk] = jnp.zeros((chunk - length, width), f32)

    @pl.when(ax != last_ax)
    def _():
        first.wait()
        supply.wait()
        factor.wait()
        turned = rate[...].T
        for q in range(pairs):
            at = pl.multiple_of((q ^ place) * chunk, SUB)
            even = turned[:, 2 * q : 2 * q + 1] * plenum[2 * q]
            odd = turned[:, 2 * q + 1 : 2 * q + 2] * plenum[2 * q + 1]
            own = jnp.where(parity == 0, even, odd)
            other = jnp.where(parity == 0, odd, even)
            for p in range(2):
                rows = pl.ds(pl.multiple_of(at + p * slots, SUB), slots)
                keep[rows] = jnp.where(parity == p, own, 0.0)
                send[rows] = jnp.where(parity == p, other, 0.0)
            if chunk > 2 * slots:
                rest = pl.ds(pl.multiple_of(at + 2 * slots, SUB), chunk - 2 * slots)
                keep[rest] = jnp.zeros((chunk - 2 * slots, width), f32)
                send[rest] = jnp.zeros((chunk - 2 * slots, width), f32)

    lane = lax.broadcasted_iota(jnp.int32, (SUB, LANES), 1)
    halves = depth // SUB
    for e, (_, by) in enumerate(sides):
        edges[e].wait()
        for g in range(column.shape[1]):
            acc = jnp.zeros((SUB, LANES), f32)
            for j in range(LANES):
                c, rest = divmod(g * LANES + j, cells * halves)
                t, h = divmod(rest, halves)
                piece = tile[e, c, t, h * SUB : (h + 1) * SUB, :]
                acc = jnp.where(lane == j, pltpu.roll(piece, by(j), 1), acc)
            column[e, g] = acc
    for one in copies:
        one.wait()
    face.wait()


def stencil(source, swirl, mask, flags, near, column_low, column_high, out, fields, levels, sem):
    azi, rad = lax.axis_index("azi"), lax.axis_index("rad")
    last_rad = lax.axis_size("rad") - 1
    count, cells, depth, width = fields.shape
    base = near.shape[0] - count * depth
    parity = azi % 2
    halves = depth // SUB
    blocks = width // LANES
    lane = lax.broadcasted_iota(jnp.int32, (SUB, LANES), 1)
    row = lax.broadcasted_iota(jnp.int32, (SUB, LANES), 0)
    at_left, at_right = lane == 0, lane == LANES - 1
    at_low, at_high = row == 0, row == SUB - 1
    has_left, has_right = rad > 0, rad < last_rad
    pieces = [slice(k * TILE, (k + 1) * TILE) for k in range(cells // TILE)]
    copies = [pltpu.make_async_copy(source.at[:, p], fields.at[:, p], sem.at[k]) for k, p in enumerate(pieces)]
    for copy in copies:
        copy.start()
    turned = (0.5 * flags[...].astype(f32)).T
    for k in range(cells // TILE):
        levels[k] = jnp.broadcast_to(turned[:, k : k + 1], (depth, LANES))

    def cut(h, l):
        return slice(h * SUB, (h + 1) * SUB), slice(l * LANES, (l + 1) * LANES)

    def slab(t, before, after):
        level = levels[t // TILE]
        for c in range(count):
            edges = []
            for h in range(halves):
                n = (c * cells + t) * halves + h
                g, j = n // LANES, n % LANES
                edges.append((
                    jnp.where(has_left, pltpu.roll(column_low[g], (LANES - j) % LANES, 1), 0.0),
                    jnp.where(has_right, pltpu.roll(column_high[g], LANES - 1 - j, 1), 0.0),
                ))
            parts = [[fields[(c, t) + cut(h, l)] for l in range(blocks)] for h in range(halves)]
            ups = [[pltpu.roll(v, 1, 1) for v in p] for p in parts]
            downs = [[pltpu.roll(v, LANES - 1, 1) for v in p] for p in parts]
            for l in range(blocks):
                lows = [pltpu.roll(parts[h][l], 1, 0) for h in range(halves)]
                highs = [pltpu.roll(parts[h][l], SUB - 1, 0) for h in range(halves)]
                for h in range(halves):
                    left = jnp.where(at_left, ups[h][l - 1] if l else edges[h][0], ups[h][l])
                    right = jnp.where(at_right, downs[h][l + 1] if l + 1 < blocks else edges[h][1], downs[h][l])
                    low = jnp.where(at_low, lows[h - 1] if h else 0.0, lows[h])
                    high = jnp.where(at_high, highs[h + 1] if h + 1 < halves else 0.0, highs[h])
                    total = (left + right) + (low + high) + after(c, h, l)
                    speed = swirl[(t,) + cut(h, l)]
                    value = parts[h][l] * (0.4 - speed) + before(c, h, l) * (speed + 0.1) + 0.1 * total
                    if c == 0:
                        out[(0, t) + cut(h, l)] = value
                    else:
                        live = jnp.where(mask[(t,) + cut(h, l)] == 0, level[h * SUB : (h + 1) * SUB], 0.0) * parts[h][l]
                        energy = fields[(0, t) + cut(h, l)]
                        burn = live + live * jnp.tanh(2.0 * energy - 1.0)
                        out[(0, t) + cut(h, l)] += burn
                        out[(1, t) + cut(h, l)] = value - 0.5 * burn

    def halo(use_near):
        def value(c, h, l):
            _, lanes = cut(h, l)
            first = base + c * depth + h * SUB
            return jnp.where(use_near, near[first : first + SUB, lanes], 0.0)

        return value

    def inside(t):
        return lambda c, h, l: fields[(c, t) + cut(h, l)]

    def step(t, carry):
        slab(t, inside(t - 1), inside(t + 1))
        return carry

    copies[0].wait()
    slab(0, halo(parity == 1), inside(1))
    for k, copy in enumerate(copies):
        if k:
            copy.wait()
        lax.fori_loop(k * TILE - 1 if k else 1, (k + 1) * TILE - 1, step, 0, unroll=UNROLL)
    slab(cells - 1, inside(cells - 2), halo(parity == 0))


def feed_rows(slots, targets, *refs):
    *arrived, feed = refs
    place = lax.axis_index("azi") // 2
    rows = feed.shape[0] - SUB
    feed[...] = jnp.zeros(feed.shape, f32)

    @pl.when(lax.axis_index("ax") == 0)
    def _():
        for k, block in enumerate(arrived):
            for p in range(2):
                for j in range(slots):
                    target = targets[2 * (place ^ k) + p, j]
                    at = jnp.where(target >= 0, target // HEAD * SUB + target % HEAD, rows)
                    r = p * slots + j
                    feed[pl.ds(at, 1), :] += block[r : r + 1, :]


def finish(chunk, length, far, speed, axial_low, axial_high, row_top, own, other, weights, feed, before, out, modes, high, result, sem):
    azi, ax = lax.axis_index("azi"), lax.axis_index("ax")
    last_ax = lax.axis_size("ax") - 1
    count, cells, depth, width = before.shape
    parity = azi % 2
    pairs = own.shape[0] // chunk

    @pl.when(ax == last_ax)
    def _():
        for k in range(pairs):
            for ref, p in ((own, parity), (other, 1 - parity)):
                at = pl.multiple_of((2 * k + p) * length, SUB)
                modes[pl.ds(at, length)] = ref[k * chunk : k * chunk + length]
        per = modes.shape[0] // count
        for c in range(count):
            rebuilt = jnp.dot(
                weights[c], modes[c * per : (c + 1) * per], precision=HIGH, preferred_element_type=f32
            )
            high[c] = 0.1 * row_top[c] - rebuilt

    @pl.when(ax != last_ax)
    def _():
        for c in range(count):
            high[c] = 0.1 * axial_high[c]

    scale = jnp.where(ax > 0, 0.1, 0.0)
    row = lax.broadcasted_iota(jnp.int32, (SUB, width), 0)
    group = SUB
    copies = []
    for b in range(cells // group):
        for c in range(count):
            low_rows = scale * axial_low[c, b * group : (b + 1) * group]
            high_rows = high[c, b * group : (b + 1) * group]
            for i in range(group):
                t = b * group + i
                head = before[c, t, :SUB] + jnp.where(row == 0, low_rows[i : i + 1], 0.0)
                if c == 1:
                    head = head + feed[t * SUB : (t + 1) * SUB]
                result[c, t, :SUB] = head
                if depth > 2 * SUB:
                    result[c, t, SUB : depth - SUB] = before[c, t, SUB : depth - SUB]
                tail = before[c, t, depth - SUB :]
                result[c, t, depth - SUB :] = tail + jnp.where(row == SUB - 1, high_rows[i : i + 1], 0.0)
                if t in (0, cells - 1):
                    layer = far[c * depth : (c + 1) * depth]
                    if t:
                        result[c, t] += jnp.where(parity == 1, 0.1 * layer, 0.0)
                    else:
                        result[c, t] += jnp.where(parity == 0, (speed[...] + 0.1) * layer, 0.0)
            cells_at = pl.ds(b * group, group)
            copy = pltpu.make_async_copy(result.at[c, cells_at], out.at[c, cells_at], sem.at[c, b])
            copy.start()
            copies.append(copy)
    for copy in copies:
        copy.wait()


def body(fields, swirl_speed, ghost_mask, tile_flags, outlet_gain, feed_rate, plenum, feed_target):
    sectors, radials = lax.axis_size("azi"), lax.axis_size("rad")
    count, cells, depth, width = fields.shape
    half_modes = outlet_gain.shape[1]
    modes = 2 * half_modes
    slots = plenum.shape[2]
    length = count * modes // sectors
    chunk = max(length, 2 * slots)
    pairs = sectors // 2
    total_cells = cells * sectors
    phase, phase_t = phases(total_cells, lax.axis_index("azi") * cells, cells, half_modes)
    gain = jnp.concatenate([outlet_gain, outlet_gain], axis=1)
    weights = phase_t[None] * gain[:, None, :] * (0.1 * 2.0 / math.sqrt(half_modes * total_cells))
    groups = count * cells * depth // SUB // LANES

    struct = jax.ShapeDtypeStruct
    keep, send, shift, row_top, row_out, column = pl.pallas_call(
        functools.partial(prepare, chunk),
        out_shape=(
            struct((pairs * chunk, width), f32),
            struct((pairs * chunk + count * depth, width), f32),
            struct((count * depth, width), f32),
            struct((count, cells, width), f32),
            struct((count, cells, width), f32),
            struct((1 if radials == 2 else 2, groups, SUB, LANES), f32),
        ),
        in_specs=[HBM, VMEM, HBM, HBM],
        out_specs=[VMEM] * 6,
        scratch_shapes=[
            pltpu.VMEM((sectors, slots), f32),
            pltpu.VMEM((sectors, slots, width), f32),
            pltpu.VMEM((1 if radials == 2 else 2, count, cells, depth, LANES), f32),
            pltpu.SemaphoreType.DMA((2 * count + 7,)),
        ],
        compiler_params=params(12),
        cost_estimate=cost(1 << 26, 1 << 21),
        name="prepare",
    )(in_hbm(fields), phase, in_hbm(feed_rate[0]), in_hbm(plenum[0]))

    def swap(x, k):
        return lax.ppermute(x, "azi", [(i, i ^ k) for i in range(sectors)])

    def across(axis, to_high, to_low, to_only):
        size = lax.axis_size(axis)
        if size == 2:
            received = lax.ppermute(to_only, axis, [(0, 1), (1, 0)])
            return received, received
        ups = [(i, i + 1) for i in range(size - 1)]
        return lax.ppermute(to_high, axis, ups), lax.ppermute(to_low, axis, [(b, a) for a, b in ups])

    offset = [(i, (i + 1) % sectors if i % 2 else (i - 1) % sectors) for i in range(sectors)]
    near = swap(send, 1)
    far = lax.ppermute(shift, "azi", offset)
    axial_low, axial_high = across("ax", row_top, row_out, row_out)
    edge_low, edge_high = across("rad", column[0], column[-1], column[0])

    mixed = keep + near[: pairs * chunk]
    parts = [mixed[k * chunk : (k + 1) * chunk] for k in range(pairs)]
    arrived = [mixed]
    for k in range(1, pairs):
        arrived.append(swap(jnp.concatenate(parts[k:] + parts[:k], axis=0), 2 * k))
    summed = functools.reduce(
        jnp.add, [mixed] + [jnp.concatenate([x[(pairs - k) * chunk :], x[: (pairs - k) * chunk]], axis=0) for k, x in enumerate(arrived) if k]
    )

    before = pl.pallas_call(
        stencil,
        out_shape=struct(fields.shape, f32),
        in_specs=[HBM] + [VMEM] * 6,
        out_specs=VMEM,
        scratch_shapes=[
            pltpu.VMEM(fields.shape, f32),
            pltpu.VMEM((cells // TILE, depth, LANES), f32),
            pltpu.SemaphoreType.DMA((cells // TILE,)),
        ],
        compiler_params=params(12),
        cost_estimate=cost(1 << 28, 1 << 23),
        name="stencil",
    )(in_hbm(fields), swirl_speed, ghost_mask, tile_flags, near, edge_low, edge_high)

    feed = pl.pallas_call(
        functools.partial(feed_rows, slots),
        out_shape=struct((cells * SUB + SUB, width), f32),
        in_specs=[SMEM] + [VMEM] * pairs,
        out_specs=VMEM,
        compiler_params=params(8),
        cost_estimate=cost(1 << 25, 1 << 20),
        name="feed",
    )(feed_target[0], *arrived)

    other = swap(summed, 1)

    return pl.pallas_call(
        functools.partial(finish, chunk, length),
        out_shape=struct(fields.shape, f32),
        in_specs=[VMEM] * 10,
        out_specs=HBM,
        scratch_shapes=[
            pltpu.VMEM((count * modes, width), f32),
            pltpu.VMEM((count, cells, width), f32),
            pltpu.VMEM(fields.shape, f32),
            pltpu.SemaphoreType.DMA((count, cells // SUB)),
        ],
        compiler_params=params(16),
        cost_estimate=cost(1 << 26, 1 << 23),
        name="finish",
    )(far, swirl_speed[0], axial_low, axial_high, row_top, summed, other, weights, feed, before)


def solution(mesh):
    return jax.shard_map(
        body,
        mesh=mesh,
        in_specs=(
            P(None, "azi", "ax", "rad"),
            P("azi", "ax", "rad"),
            P("azi", "ax", "rad"),
            P("azi", "ax"),
            P(),
            P("azi", None, None),
            P("azi", None, None, "rad"),
            P("azi", None, None),
        ),
        out_specs=P(None, "azi", "ax", "rad"),
        check_vma=False,
    )
```

```python
import functools
import math

import jax
import jax.numpy as jnp
from jax import lax
from jax.experimental import pallas as pl
from jax.experimental.pallas import tpu as pltpu
from jax.sharding import PartitionSpec as P


TILE = 16
HEAD = 4
LANES = 128
UNROLL = 4
SUB = 8
HIGH = lax.Precision.HIGHEST
VMEM = pl.BlockSpec(memory_space=pltpu.VMEM)
SMEM = pl.BlockSpec(memory_space=pltpu.SMEM)
HBM = pl.BlockSpec(memory_space=pltpu.HBM)
f32 = jnp.float32


def params(mib):
    return pltpu.CompilerParams(vmem_limit_bytes=mib << 20)


def cost(flops, size):
    return pl.CostEstimate(flops=flops, bytes_accessed=size, transcendentals=0)


def in_hbm(x):
    return pltpu.with_memory_space_constraint(x, pltpu.HBM)


def phases(length, first_cell, cell_count, mode_count):
    cells = first_cell + jnp.arange(cell_count, dtype=jnp.int32)
    order = jnp.arange(1, mode_count + 1, dtype=jnp.int32)
    angle = (order[:, None] * cells[None, :] % length).astype(f32) * (2.0 * math.pi / length)
    turned = (cells[:, None] * order[None, :] % length).astype(f32) * (2.0 * math.pi / length)
    return (
        jnp.concatenate([jnp.cos(angle), jnp.sin(angle)], axis=0),
        jnp.concatenate([jnp.cos(turned), jnp.sin(turned)], axis=1),
    )


def prepare(
    chunk, fields, phase, rates, profile, keep, send, shift, row_top, row_out, column, rate, plenum, tile, sem
):
    azi, ax, rad = lax.axis_index("azi"), lax.axis_index("ax"), lax.axis_index("rad")
    last_ax = lax.axis_size("ax") - 1
    count, cells, depth, width = fields.shape
    sectors, slots, _ = profile.shape
    pairs = sectors // 2
    parity, place = azi % 2, azi // 2
    base = pairs * chunk
    t_pair = jnp.where(parity == 0, cells - 1, 0)
    t_shift = jnp.where(parity == 0, 0, cells - 1)
    row_sent = jnp.where((ax == 0) & (last_ax == 1), depth - 1, 0)
    if lax.axis_size("rad") == 2:
        more = jnp.where(rad == 0, 1, 0)
        sides = [(jnp.where(rad == 0, width - LANES, 0), lambda j: (j + more) if j < LANES - 1 else j * (1 - more))]
    else:
        sides = [(width - LANES, lambda j: (j + 1) % LANES), (0, lambda j: j)]
    first = pltpu.make_async_copy(fields.at[:, :, depth - 1, :], row_top, sem.at[0])
    first.start()
    copies = []
    for c in range(count):
        rows = slice(base + c * depth, base + (c + 1) * depth)
        copies.append(pltpu.make_async_copy(fields.at[c, t_pair], send.at[rows], sem.at[1 + 2 * c]))
        rows = slice(c * depth, (c + 1) * depth)
        copies.append(pltpu.make_async_copy(fields.at[c, t_shift], shift.at[rows], sem.at[2 + 2 * c]))
    edges = [
        pltpu.make_async_copy(
            fields.at[:, :, :, pl.ds(pl.multiple_of(side, LANES), LANES)], tile.at[e], sem.at[5 + 2 * count + e]
        )
        for e, (side, _) in enumerate(sides)
    ]
    for one in copies:
        one.start()
    for edge in edges:
        edge.start()
    face = pltpu.make_async_copy(fields.at[:, :, row_sent, :], row_out, sem.at[2 + 2 * count])
    face.start()
    supply = pltpu.make_async_copy(profile, plenum, sem.at[3 + 2 * count])
    supply.start()
    factor = pltpu.make_async_copy(rates, rate, sem.at[4 + 2 * count])
    factor.start()

    @pl.when(ax == last_ax)
    def _():
        first.wait()
        supply.wait()
        factor.wait()
        sums = [
            jnp.dot(phase[...], row_top[c], precision=HIGH, preferred_element_type=f32)
            for c in range(count)
        ]
        modes = phase.shape[0]
        length = count * modes // sectors
        blocks = []
        for s in range(sectors):
            c, m = divmod(s * length, modes)
            blocks.append(sums[c][m : m + length])
        for q in range(pairs):
            even, odd = blocks[2 * q], blocks[2 * q + 1]
            at = q * chunk
            keep[at : at + length] = jnp.where(parity == 0, even, odd)
            send[at : at + length] = jnp.where(parity == 0, odd, even)
            if chunk > length:
                keep[at + length : at + chunk] = jnp.zeros((chunk - length, width), f32)
                send[at + length : at + chunk] = jnp.zeros((chunk - length, width), f32)

    @pl.when(ax != last_ax)
    def _():
        first.wait()
        supply.wait()
        factor.wait()
        turned = rate[...].T
        for q in range(pairs):
            at = pl.multiple_of((q ^ place) * chunk, SUB)
            even = turned[:, 2 * q : 2 * q + 1] * plenum[2 * q]
            odd = turned[:, 2 * q + 1 : 2 * q + 2] * plenum[2 * q + 1]
            own = jnp.where(parity == 0, even, odd)
            other = jnp.where(parity == 0, odd, even)
            for p in range(2):
                rows = pl.ds(pl.multiple_of(at + p * slots, SUB), slots)
                keep[rows] = jnp.where(parity == p, own, 0.0)
                send[rows] = jnp.where(parity == p, other, 0.0)
            if chunk > 2 * slots:
                rest = pl.ds(pl.multiple_of(at + 2 * slots, SUB), chunk - 2 * slots)
                keep[rest] = jnp.zeros((chunk - 2 * slots, width), f32)
                send[rest] = jnp.zeros((chunk - 2 * slots, width), f32)

    lane = lax.broadcasted_iota(jnp.int32, (SUB, LANES), 1)
    halves = depth // SUB
    for e, (_, by) in enumerate(sides):
        edges[e].wait()
        for g in range(column.shape[1]):
            acc = jnp.zeros((SUB, LANES), f32)
            for j in range(LANES):
                c, rest = divmod(g * LANES + j, cells * halves)
                t, h = divmod(rest, halves)
                piece = tile[e, c, t, h * SUB : (h + 1) * SUB, :]
                acc = jnp.where(lane == j, pltpu.roll(piece, by(j), 1), acc)
            column[e, g] = acc
    for one in copies:
        one.wait()
    face.wait()


def stencil(begin, end, source, swirl, inert, flags, near, column_low, column_high, out, rows, mask, levels, sem):
    azi, rad = lax.axis_index("azi"), lax.axis_index("rad")
    last_rad = lax.axis_size("rad") - 1
    count, cells, depth, width = source.shape
    base = near.shape[0] - count * depth
    parity = azi % 2
    halves = depth // SUB
    blocks = width // LANES
    lane = lax.broadcasted_iota(jnp.int32, (SUB, LANES), 1)
    row = lax.broadcasted_iota(jnp.int32, (SUB, LANES), 0)
    at_left, at_right = lane == 0, lane == LANES - 1
    at_low, at_high = row == 0, row == SUB - 1
    has_left, has_right = rad > 0, rad < last_rad
    low_row, high_row = max(begin - 1, 0), min(end + 1, cells)
    middle = begin + (end - begin) // 2
    cuts = [low_row, middle + 1, high_row]
    copies = []
    for k, (a, b) in enumerate(zip(cuts, cuts[1:])):
        piece = rows.at[:, a - low_row : b - low_row]
        copies.append(pltpu.make_async_copy(source.at[:, a:b], piece, sem.at[k]))
    for k, (a, b) in enumerate(((begin, middle), (middle, end))):
        copies.append(pltpu.make_async_copy(inert.at[a:b], mask.at[a - begin : b - begin], sem.at[2 + k]))
    for k in (0, 2, 1, 3):
        copies[k].start()
    turned = (0.5 * flags[...].astype(f32)).T
    for k in range(cells // TILE):
        levels[k] = jnp.broadcast_to(turned[:, k : k + 1], (depth, LANES))

    def cut(h, l):
        return slice(h * SUB, (h + 1) * SUB), slice(l * LANES, (l + 1) * LANES)

    def slab(t, before, after):
        level = levels[t // TILE]
        for c in range(count):
            edges = []
            for h in range(halves):
                n = (c * cells + t) * halves + h
                g, j = n // LANES, n % LANES
                edges.append((
                    jnp.where(has_left, pltpu.roll(column_low[g], (LANES - j) % LANES, 1), 0.0),
                    jnp.where(has_right, pltpu.roll(column_high[g], LANES - 1 - j, 1), 0.0),
                ))
            parts = [[rows[(c, t - low_row) + cut(h, l)] for l in range(blocks)] for h in range(halves)]
            ups = [[pltpu.roll(v, 1, 1) for v in p] for p in parts]
            downs = [[pltpu.roll(v, LANES - 1, 1) for v in p] for p in parts]
            for l in range(blocks):
                lows = [pltpu.roll(parts[h][l], 1, 0) for h in range(halves)]
                highs = [pltpu.roll(parts[h][l], SUB - 1, 0) for h in range(halves)]
                for h in range(halves):
                    left = jnp.where(at_left, ups[h][l - 1] if l else edges[h][0], ups[h][l])
                    right = jnp.where(at_right, downs[h][l + 1] if l + 1 < blocks else edges[h][1], downs[h][l])
                    low = jnp.where(at_low, lows[h - 1] if h else 0.0, lows[h])
                    high = jnp.where(at_high, highs[h + 1] if h + 1 < halves else 0.0, highs[h])
                    total = (left + right) + (low + high) + after(c, h, l)
                    speed = swirl[(t,) + cut(h, l)]
                    value = parts[h][l] * (0.4 - speed) + before(c, h, l) * (speed + 0.1) + 0.1 * total
                    if c == 0:
                        out[(0, t - begin) + cut(h, l)] = value
                    else:
                        live = jnp.where(mask[(t - begin,) + cut(h, l)] == 0, level[h * SUB : (h + 1) * SUB], 0.0) * parts[h][l]
                        energy = rows[(0, t - low_row) + cut(h, l)]
                        burn = live + live * jnp.tanh(2.0 * energy - 1.0)
                        out[(0, t - begin) + cut(h, l)] += burn
                        out[(1, t - begin) + cut(h, l)] = value - 0.5 * burn

    def halo(use_near):
        def value(c, h, l):
            _, lanes = cut(h, l)
            first = base + c * depth + h * SUB
            return jnp.where(use_near, near[first : first + SUB, lanes], 0.0)

        return value

    def inside(t):
        return lambda c, h, l: rows[(c, t - low_row) + cut(h, l)]

    def step(t, carry):
        slab(t, inside(t - 1), inside(t + 1))
        return carry

    copies[0].wait()
    copies[2].wait()
    if begin == 0:
        slab(0, halo(parity == 1), inside(1))
    lax.fori_loop(max(begin, 1), middle, step, 0, unroll=UNROLL)
    copies[1].wait()
    copies[3].wait()
    lax.fori_loop(middle, min(end, cells - 1), step, 0, unroll=UNROLL)
    if end == cells:
        slab(cells - 1, inside(cells - 2), halo(parity == 0))


def feed_rows(slots, targets, *refs):
    *arrived, feed = refs
    place = lax.axis_index("azi") // 2
    rows = feed.shape[0] - SUB
    feed[...] = jnp.zeros(feed.shape, f32)

    @pl.when(lax.axis_index("ax") == 0)
    def _():
        for k, block in enumerate(arrived):
            for p in range(2):
                for j in range(slots):
                    target = targets[2 * (place ^ k) + p, j]
                    at = jnp.where(target >= 0, target // HEAD * SUB + target % HEAD, rows)
                    r = p * slots + j
                    feed[pl.ds(at, 1), :] += block[r : r + 1, :]


def finish(chunk, length, far, speed, axial_low, axial_high, row_top, own, other, weights, feed, before_a, before_b, out, modes, high, result, sem):
    azi, ax = lax.axis_index("azi"), lax.axis_index("ax")
    last_ax = lax.axis_size("ax") - 1
    count, cells, depth, width = result.shape
    parity, fold = azi % 2, azi // 2 % 2
    pairs = own.shape[0] // chunk
    split = before_a.shape[1]

    @pl.when(ax == last_ax)
    def _():
        for k in range(pairs):
            j, same = k % (pairs // 2), k < pairs // 2
            chip = 2 * j + (fold if same else 1 - fold)
            for ref, p in ((own, parity), (other, 1 - parity)):
                at = pl.multiple_of((2 * chip + p) * length, SUB)
                modes[pl.ds(at, length)] = ref[k * chunk : k * chunk + length]
        per = modes.shape[0] // count
        for c in range(count):
            rebuilt = jnp.dot(
                weights[c], modes[c * per : (c + 1) * per], precision=HIGH, preferred_element_type=f32
            )
            high[c] = 0.1 * row_top[c] - rebuilt

    @pl.when(ax != last_ax)
    def _():
        for c in range(count):
            high[c] = 0.1 * axial_high[c]

    scale = jnp.where(ax > 0, 0.1, 0.0)
    row = lax.broadcasted_iota(jnp.int32, (SUB, width), 0)
    group = SUB
    copies = []
    for b in range(cells // group):
        for c in range(count):
            low_rows = scale * axial_low[c, b * group : (b + 1) * group]
            high_rows = high[c, b * group : (b + 1) * group]
            for i in range(group):
                t = b * group + i
                before, u = (before_a, t) if t < split else (before_b, t - split)
                head = before[c, u, :SUB] + jnp.where(row == 0, low_rows[i : i + 1], 0.0)
                if c == 1:
                    head = head + feed[t * SUB : (t + 1) * SUB]
                result[c, t, :SUB] = head
                if depth > 2 * SUB:
                    result[c, t, SUB : depth - SUB] = before[c, u, SUB : depth - SUB]
                tail = before[c, u, depth - SUB :]
                result[c, t, depth - SUB :] = tail + jnp.where(row == SUB - 1, high_rows[i : i + 1], 0.0)
                if t in (0, cells - 1):
                    layer = far[c * depth : (c + 1) * depth]
                    if t:
                        result[c, t] += jnp.where(parity == 1, 0.1 * layer, 0.0)
                    else:
                        result[c, t] += jnp.where(parity == 0, (speed[...] + 0.1) * layer, 0.0)
            cells_at = pl.ds(b * group, group)
            copy = pltpu.make_async_copy(result.at[c, cells_at], out.at[c, cells_at], sem.at[c, b])
            copy.start()
            copies.append(copy)
    for copy in copies:
        copy.wait()


def body(fields, swirl_speed, ghost_mask, tile_flags, outlet_gain, feed_rate, plenum, feed_target):
    sectors, slabs, radials = lax.axis_size("azi"), lax.axis_size("ax"), lax.axis_size("rad")
    count, cells, depth, width = fields.shape
    half_modes = outlet_gain.shape[1]
    modes = 2 * half_modes
    slots = plenum.shape[2]
    length = count * modes // sectors
    chunk = max(length, 2 * slots)
    pairs = sectors // 2
    total_cells = cells * sectors
    phase, phase_t = phases(total_cells, lax.axis_index("azi") * cells, cells, half_modes)
    gain = jnp.concatenate([outlet_gain, outlet_gain], axis=1)
    weights = phase_t[None] * gain[:, None, :] * (0.1 * 2.0 / math.sqrt(half_modes * total_cells))
    groups = count * cells * depth // SUB // LANES

    struct = jax.ShapeDtypeStruct
    keep, send, shift, row_top, row_out, column = pl.pallas_call(
        functools.partial(prepare, chunk),
        out_shape=(
            struct((pairs * chunk, width), f32),
            struct((pairs * chunk + count * depth, width), f32),
            struct((count * depth, width), f32),
            struct((count, cells, width), f32),
            struct((count, cells, width), f32),
            struct((1 if radials == 2 else 2, groups, SUB, LANES), f32),
        ),
        in_specs=[HBM, VMEM, HBM, HBM],
        out_specs=[VMEM] * 6,
        scratch_shapes=[
            pltpu.VMEM((sectors, slots), f32),
            pltpu.VMEM((sectors, slots, width), f32),
            pltpu.VMEM((1 if radials == 2 else 2, count, cells, depth, LANES), f32),
            pltpu.SemaphoreType.DMA((2 * count + 7,)),
        ],
        compiler_params=params(12),
        cost_estimate=cost(1 << 26, 1 << 21),
        name="prepare",
    )(in_hbm(fields), phase, in_hbm(feed_rate[0]), in_hbm(plenum[0]))

    def swap(x, k):
        return lax.ppermute(x, "azi", [(i, i ^ k) for i in range(sectors)])

    def across(axis, to_high, to_low, to_only):
        size = lax.axis_size(axis)
        if size == 2:
            received = lax.ppermute(to_only, axis, [(0, 1), (1, 0)])
            return received, received
        ups = [(i, i + 1) for i in range(size - 1)]
        return lax.ppermute(to_high, axis, ups), lax.ppermute(to_low, axis, [(b, a) for a, b in ups])

    offset = [(i, (i + 1) % sectors if i % 2 else (i - 1) % sectors) for i in range(sectors)]
    near = swap(send, 1)
    far = lax.ppermute(shift, "azi", offset)
    axial_low, axial_high = across("ax", row_top, row_out, row_out)
    edge_low, edge_high = across("rad", column[0], column[-1], column[0])

    mixed = keep + near[: pairs * chunk]
    parts = [mixed[k * chunk : (k + 1) * chunk] for k in range(pairs)]
    is_outlet = lax.axis_index("ax") == slabs - 1
    low_bit = lax.axis_index("azi") // 2 % 2
    even, odd = jnp.concatenate(parts[::2], axis=0), jnp.concatenate(parts[1::2], axis=0)

    def carry(modes_part, k):
        return jnp.where(is_outlet, modes_part, jnp.concatenate([parts[k]] * (pairs // 2), axis=0))

    folded = swap(carry(jnp.where(low_bit == 0, odd, even), 1), 2)
    half = jnp.where(low_bit == 0, even, odd) + folded
    half, *outgoing = lax.optimization_barrier([half] + [carry(half, k) for k in range(1, pairs)])
    arrived = [half]
    for k, block in enumerate(outgoing, 1):
        arrived.append(swap(block, 2 * k))
    arrived = lax.optimization_barrier(arrived)
    summed = jnp.concatenate(
        [functools.reduce(jnp.add, arrived[0::2]), functools.reduce(jnp.add, arrived[1::2])], axis=0
    )
    profiles = [parts[0], folded] + arrived[2:]

    split = cells // 2 + 1
    befores = []
    for begin, end in ((0, split), (split, cells)):
        befores.append(
            pl.pallas_call(
                functools.partial(stencil, begin, end),
                out_shape=struct((count, end - begin, depth, width), f32),
                in_specs=[HBM, VMEM, HBM] + [VMEM] * 4,
                out_specs=VMEM,
                scratch_shapes=[
                    pltpu.VMEM((count, end - begin + 1, depth, width), f32),
                    pltpu.VMEM((end - begin, depth, width), jnp.int32),
                    pltpu.VMEM((cells // TILE, depth, LANES), f32),
                    pltpu.SemaphoreType.DMA((4,)),
                ],
                compiler_params=params(8),
                cost_estimate=cost(1 << 27, 1 << 22),
            )(in_hbm(fields), swirl_speed, in_hbm(ghost_mask), tile_flags, near, edge_low, edge_high)
        )

    feed = pl.pallas_call(
        functools.partial(feed_rows, slots),
        out_shape=struct((cells * SUB + SUB, width), f32),
        in_specs=[SMEM] + [VMEM] * pairs,
        out_specs=VMEM,
        compiler_params=params(8),
        cost_estimate=cost(1 << 25, 1 << 20),
        name="feed",
    )(feed_target[0], *profiles)

    other = swap(summed, 1)

    return pl.pallas_call(
        functools.partial(finish, chunk, length),
        out_shape=struct(fields.shape, f32),
        in_specs=[VMEM] * 11,
        out_specs=HBM,
        scratch_shapes=[
            pltpu.VMEM((count * modes, width), f32),
            pltpu.VMEM((count, cells, width), f32),
            pltpu.VMEM(fields.shape, f32),
            pltpu.SemaphoreType.DMA((count, cells // SUB)),
        ],
        compiler_params=params(16),
        cost_estimate=cost(1 << 26, 1 << 23),
        name="finish",
    )(far, swirl_speed[0], axial_low, axial_high, row_top, summed, other, weights, feed, *befores)


def solution(mesh):
    return jax.shard_map(
        body,
        mesh=mesh,
        in_specs=(
            P(None, "azi", "ax", "rad"),
            P("azi", "ax", "rad"),
            P("azi", "ax", "rad"),
            P("azi", "ax"),
            P(),
            P("azi", None, None),
            P("azi", None, None, "rad"),
            P("azi", None, None),
        ),
        out_specs=P(None, "azi", "ax", "rad"),
        check_vma=False,
    )
```

```python
import functools
import math

import jax
import jax.numpy as jnp
from jax import lax
from jax.experimental import pallas as pl
from jax.experimental.pallas import tpu as pltpu
from jax.sharding import PartitionSpec as P


TILE = 16
HEAD = 4
LANES = 128
UNROLL = 4
SUB = 8
HIGH = lax.Precision.HIGHEST
VMEM = pl.BlockSpec(memory_space=pltpu.VMEM)
SMEM = pl.BlockSpec(memory_space=pltpu.SMEM)
HBM = pl.BlockSpec(memory_space=pltpu.HBM)
f32 = jnp.float32


def params(mib):
    return pltpu.CompilerParams(vmem_limit_bytes=mib << 20)


def cost(flops, size):
    return pl.CostEstimate(flops=flops, bytes_accessed=size, transcendentals=0)


def in_hbm(x):
    return pltpu.with_memory_space_constraint(x, pltpu.HBM)


def phases(length, first_cell, cell_count, mode_count):
    cells = first_cell + jnp.arange(cell_count, dtype=jnp.int32)
    order = jnp.arange(1, mode_count + 1, dtype=jnp.int32)
    angle = (order[:, None] * cells[None, :] % length).astype(f32) * (2.0 * math.pi / length)
    turned = (cells[:, None] * order[None, :] % length).astype(f32) * (2.0 * math.pi / length)
    return (
        jnp.concatenate([jnp.cos(angle), jnp.sin(angle)], axis=0),
        jnp.concatenate([jnp.cos(turned), jnp.sin(turned)], axis=1),
    )


def prepare(
    chunk, fields, phase, rates, profile, keep, send, shift, row_top, row_out, tile, rate, plenum, sem
):
    azi, ax = lax.axis_index("azi"), lax.axis_index("ax")
    last_ax = lax.axis_size("ax") - 1
    count, cells, depth, width = fields.shape
    sectors, slots, _ = profile.shape
    pairs = sectors // 2
    parity, place = azi % 2, azi // 2
    base = pairs * chunk
    t_pair = jnp.where(parity == 0, cells - 1, 0)
    t_shift = jnp.where(parity == 0, 0, cells - 1)
    row_sent = jnp.where((ax == 0) & (last_ax == 1), depth - 1, 0)
    first = pltpu.make_async_copy(fields.at[:, :, depth - 1, :], row_top, sem.at[0])
    first.start()
    copies = []
    for c in range(count):
        rows = slice(base + c * depth, base + (c + 1) * depth)
        copies.append(pltpu.make_async_copy(fields.at[c, t_pair], send.at[rows], sem.at[1 + 2 * c]))
        rows = slice(c * depth, (c + 1) * depth)
        copies.append(pltpu.make_async_copy(fields.at[c, t_shift], shift.at[rows], sem.at[2 + 2 * c]))
    for one in copies:
        one.start()
    face = pltpu.make_async_copy(fields.at[:, :, row_sent, :], row_out, sem.at[2 + 2 * count])
    face.start()
    for e, (block, _) in enumerate(columns_sent(width)):
        lanes = pl.ds(pl.multiple_of(block, LANES), LANES)
        copies.append(pltpu.make_async_copy(fields.at[:, :, :, lanes], tile.at[e], sem.at[5 + 2 * count + e]))
        copies[-1].start()
    supply = pltpu.make_async_copy(profile, plenum, sem.at[3 + 2 * count])
    supply.start()
    factor = pltpu.make_async_copy(rates, rate, sem.at[4 + 2 * count])
    factor.start()

    @pl.when(ax == last_ax)
    def _():
        first.wait()
        sums = [
            jnp.dot(phase[...], row_top[c], precision=HIGH, preferred_element_type=f32)
            for c in range(count)
        ]
        modes = phase.shape[0]
        length = count * modes // sectors
        blocks = []
        for s in range(sectors):
            c, m = divmod(s * length, modes)
            blocks.append(sums[c][m : m + length])
        for q in range(pairs):
            even, odd = blocks[2 * q], blocks[2 * q + 1]
            at = q * chunk
            keep[at : at + length] = jnp.where(parity == 0, even, odd)
            send[at : at + length] = jnp.where(parity == 0, odd, even)
            if chunk > length:
                keep[at + length : at + chunk] = jnp.zeros((chunk - length, width), f32)
                send[at + length : at + chunk] = jnp.zeros((chunk - length, width), f32)

    supply.wait()
    factor.wait()

    @pl.when(ax != last_ax)
    def _():
        first.wait()
        turned = rate[...].T
        for q in range(pairs):
            at = pl.multiple_of((q ^ place) * chunk, SUB)
            even = turned[:, 2 * q : 2 * q + 1] * plenum[2 * q]
            odd = turned[:, 2 * q + 1 : 2 * q + 2] * plenum[2 * q + 1]
            own = jnp.where(parity == 0, even, odd)
            other = jnp.where(parity == 0, odd, even)
            for p in range(2):
                rows = pl.ds(pl.multiple_of(at + p * slots, SUB), slots)
                keep[rows] = jnp.where(parity == p, own, 0.0)
                send[rows] = jnp.where(parity == p, other, 0.0)
            if chunk > 2 * slots:
                rest = pl.ds(pl.multiple_of(at + 2 * slots, SUB), chunk - 2 * slots)
                keep[rest] = jnp.zeros((chunk - 2 * slots, width), f32)
                send[rest] = jnp.zeros((chunk - 2 * slots, width), f32)

    for one in copies:
        one.wait()
    face.wait()


def columns_sent(width):
    if lax.axis_size("rad") != 2:
        return [(width - LANES, lambda j: (j + 1) % LANES), (0, lambda j: j)]
    more = jnp.where(lax.axis_index("rad") == 0, 1, 0)
    return [(more * (width - LANES), lambda j: (j + more) if j < LANES - 1 else j * (1 - more))]


def columns(tile, column):
    _, cells, depth = tile.shape[1:4]
    sides = columns_sent(LANES)
    lane = lax.broadcasted_iota(jnp.int32, (SUB, LANES), 1)
    halves = depth // SUB
    for e, (_, by) in enumerate(sides):
        for g in range(column.shape[1]):
            acc = jnp.zeros((SUB, LANES), f32)
            for j in range(LANES):
                c, rest = divmod(g * LANES + j, cells * halves)
                t, h = divmod(rest, halves)
                piece = tile[e, c, t, h * SUB : (h + 1) * SUB, :]
                acc = jnp.where(lane == j, pltpu.roll(piece, by(j), 1), acc)
            column[e, g] = acc


def stencil(source, swirl, mask, flags, near, column_low, column_high, out, fields, levels, sem):
    azi, rad = lax.axis_index("azi"), lax.axis_index("rad")
    last_rad = lax.axis_size("rad") - 1
    count, cells, depth, width = fields.shape
    base = near.shape[0] - count * depth
    parity = azi % 2
    halves = depth // SUB
    blocks = width // LANES
    lane = lax.broadcasted_iota(jnp.int32, (SUB, LANES), 1)
    row = lax.broadcasted_iota(jnp.int32, (SUB, LANES), 0)
    at_left, at_right = lane == 0, lane == LANES - 1
    at_low, at_high = row == 0, row == SUB - 1
    has_left, has_right = rad > 0, rad < last_rad
    pieces = [slice(k * TILE, (k + 1) * TILE) for k in range(cells // TILE)]
    copies = [pltpu.make_async_copy(source.at[:, p], fields.at[:, p], sem.at[k]) for k, p in enumerate(pieces)]
    for copy in copies:
        copy.start()
    turned = (0.5 * flags[...].astype(f32)).T
    for k in range(cells // TILE):
        levels[k] = jnp.broadcast_to(turned[:, k : k + 1], (depth, LANES))

    def cut(h, l):
        return slice(h * SUB, (h + 1) * SUB), slice(l * LANES, (l + 1) * LANES)

    def slab(t, before, after):
        level = levels[t // TILE]
        for c in range(count):
            edges = []
            for h in range(halves):
                n = (c * cells + t) * halves + h
                g, j = n // LANES, n % LANES
                edges.append((
                    jnp.where(has_left, pltpu.roll(column_low[g], (LANES - j) % LANES, 1), 0.0),
                    jnp.where(has_right, pltpu.roll(column_high[g], LANES - 1 - j, 1), 0.0),
                ))
            parts = [[fields[(c, t) + cut(h, l)] for l in range(blocks)] for h in range(halves)]
            ups = [[pltpu.roll(v, 1, 1) for v in p] for p in parts]
            downs = [[pltpu.roll(v, LANES - 1, 1) for v in p] for p in parts]
            for l in range(blocks):
                lows = [pltpu.roll(parts[h][l], 1, 0) for h in range(halves)]
                highs = [pltpu.roll(parts[h][l], SUB - 1, 0) for h in range(halves)]
                for h in range(halves):
                    left = jnp.where(at_left, ups[h][l - 1] if l else edges[h][0], ups[h][l])
                    right = jnp.where(at_right, downs[h][l + 1] if l + 1 < blocks else edges[h][1], downs[h][l])
                    low = jnp.where(at_low, lows[h - 1] if h else 0.0, lows[h])
                    high = jnp.where(at_high, highs[h + 1] if h + 1 < halves else 0.0, highs[h])
                    total = (left + right) + (low + high) + after(c, h, l)
                    speed = swirl[(t,) + cut(h, l)]
                    value = parts[h][l] * (0.4 - speed) + before(c, h, l) * (speed + 0.1) + 0.1 * total
                    if c == 0:
                        out[(0, t) + cut(h, l)] = value
                    else:
                        live = jnp.where(mask[(t,) + cut(h, l)] == 0, level[h * SUB : (h + 1) * SUB], 0.0) * parts[h][l]
                        energy = fields[(0, t) + cut(h, l)]
                        burn = live + live * jnp.tanh(2.0 * energy - 1.0)
                        out[(0, t) + cut(h, l)] += burn
                        out[(1, t) + cut(h, l)] = value - 0.5 * burn

    def halo(use_near):
        def value(c, h, l):
            _, lanes = cut(h, l)
            first = base + c * depth + h * SUB
            return jnp.where(use_near, near[first : first + SUB, lanes], 0.0)

        return value

    def inside(t):
        return lambda c, h, l: fields[(c, t) + cut(h, l)]

    def step(t, carry):
        slab(t, inside(t - 1), inside(t + 1))
        return carry

    copies[0].wait()
    slab(0, halo(parity == 1), inside(1))
    for k, copy in enumerate(copies):
        if k:
            copy.wait()
        lax.fori_loop(k * TILE - 1 if k else 1, (k + 1) * TILE - 1, step, 0, unroll=UNROLL)
    slab(cells - 1, inside(cells - 2), halo(parity == 0))


def feed_rows(slots, targets, *refs):
    *arrived, feed = refs
    place = lax.axis_index("azi") // 2
    rows = feed.shape[0] - SUB
    feed[...] = jnp.zeros(feed.shape, f32)

    @pl.when(lax.axis_index("ax") == 0)
    def _():
        for k, block in enumerate(arrived):
            for p in range(2):
                for j in range(slots):
                    target = targets[2 * (place ^ k) + p, j]
                    at = jnp.where(target >= 0, target // HEAD * SUB + target % HEAD, rows)
                    r = p * slots + j
                    feed[pl.ds(at, 1), :] += block[r : r + 1, :]


def finish(chunk, length, far, speed, axial_low, axial_high, row_top, own, other, weights, feed, before, out, modes, high, result, sem):
    azi, ax = lax.axis_index("azi"), lax.axis_index("ax")
    last_ax = lax.axis_size("ax") - 1
    count, cells, depth, width = before.shape
    parity = azi % 2
    pairs = own.shape[0] // chunk

    @pl.when(ax == last_ax)
    def _():
        for k in range(pairs):
            for ref, p in ((own, parity), (other, 1 - parity)):
                at = pl.multiple_of((2 * k + p) * length, SUB)
                modes[pl.ds(at, length)] = ref[k * chunk : k * chunk + length]
        per = modes.shape[0] // count
        for c in range(count):
            rebuilt = jnp.dot(
                weights[c], modes[c * per : (c + 1) * per], precision=HIGH, preferred_element_type=f32
            )
            high[c] = 0.1 * row_top[c] - rebuilt

    @pl.when(ax != last_ax)
    def _():
        for c in range(count):
            high[c] = 0.1 * axial_high[c]

    scale = jnp.where(ax > 0, 0.1, 0.0)
    row = lax.broadcasted_iota(jnp.int32, (SUB, width), 0)
    group = SUB
    copies = []
    for b in range(cells // group):
        for c in range(count):
            low_rows = scale * axial_low[c, b * group : (b + 1) * group]
            high_rows = high[c, b * group : (b + 1) * group]
            for i in range(group):
                t = b * group + i
                head = before[c, t, :SUB] + jnp.where(row == 0, low_rows[i : i + 1], 0.0)
                if c == 1:
                    head = head + feed[t * SUB : (t + 1) * SUB]
                result[c, t, :SUB] = head
                if depth > 2 * SUB:
                    result[c, t, SUB : depth - SUB] = before[c, t, SUB : depth - SUB]
                tail = before[c, t, depth - SUB :]
                result[c, t, depth - SUB :] = tail + jnp.where(row == SUB - 1, high_rows[i : i + 1], 0.0)
                if t in (0, cells - 1):
                    layer = far[c * depth : (c + 1) * depth]
                    if t:
                        result[c, t] += jnp.where(parity == 1, 0.1 * layer, 0.0)
                    else:
                        result[c, t] += jnp.where(parity == 0, (speed[...] + 0.1) * layer, 0.0)
            cells_at = pl.ds(b * group, group)
            copy = pltpu.make_async_copy(result.at[c, cells_at], out.at[c, cells_at], sem.at[c, b])
            copy.start()
            copies.append(copy)
    for copy in copies:
        copy.wait()


def body(fields, swirl_speed, ghost_mask, tile_flags, outlet_gain, feed_rate, plenum, feed_target):
    sectors, radials = lax.axis_size("azi"), lax.axis_size("rad")
    count, cells, depth, width = fields.shape
    half_modes = outlet_gain.shape[1]
    modes = 2 * half_modes
    slots = plenum.shape[2]
    length = count * modes // sectors
    chunk = max(length, 2 * slots)
    pairs = sectors // 2
    total_cells = cells * sectors
    phase, phase_t = phases(total_cells, lax.axis_index("azi") * cells, cells, half_modes)
    gain = jnp.concatenate([outlet_gain, outlet_gain], axis=1)
    weights = phase_t[None] * gain[:, None, :] * (0.1 * 2.0 / math.sqrt(half_modes * total_cells))
    groups = count * cells * depth // SUB // LANES

    struct = jax.ShapeDtypeStruct
    outer = 1 if radials == 2 else 2
    keep, send, shift, row_top, row_out, tile = pl.pallas_call(
        functools.partial(prepare, chunk),
        out_shape=(
            struct((pairs * chunk, width), f32),
            struct((pairs * chunk + count * depth, width), f32),
            struct((count * depth, width), f32),
            struct((count, cells, width), f32),
            struct((count, cells, width), f32),
            struct((outer, count, cells, depth, LANES), f32),
        ),
        in_specs=[HBM, VMEM, HBM, HBM],
        out_specs=[VMEM] * 6,
        scratch_shapes=[
            pltpu.VMEM((sectors, slots), f32),
            pltpu.VMEM((sectors, slots, width), f32),
            pltpu.SemaphoreType.DMA((2 * count + 7,)),
        ],
        compiler_params=params(12),
        cost_estimate=cost(1 << 26, 1 << 21),
        name="prepare",
    )(in_hbm(fields), phase, in_hbm(feed_rate[0]), in_hbm(plenum[0]))

    column = pl.pallas_call(
        columns,
        out_shape=struct((outer, groups, SUB, LANES), f32),
        in_specs=[VMEM],
        out_specs=VMEM,
        compiler_params=params(6),
        cost_estimate=cost(1 << 22, 1 << 19),
        name="columns",
    )(tile)

    def swap(x, k):
        return lax.ppermute(x, "azi", [(i, i ^ k) for i in range(sectors)])

    def across(axis, to_high, to_low, to_only):
        size = lax.axis_size(axis)
        if size == 2:
            received = lax.ppermute(to_only, axis, [(0, 1), (1, 0)])
            return received, received
        ups = [(i, i + 1) for i in range(size - 1)]
        return lax.ppermute(to_high, axis, ups), lax.ppermute(to_low, axis, [(b, a) for a, b in ups])

    offset = [(i, (i + 1) % sectors if i % 2 else (i - 1) % sectors) for i in range(sectors)]
    near = swap(send, 1)
    far = lax.ppermute(shift, "azi", offset)
    axial_low, axial_high = across("ax", row_top, row_out, row_out)
    edge_low, edge_high = across("rad", column[0], column[-1], column[0])

    mixed = keep + near[: pairs * chunk]
    parts = [mixed[k * chunk : (k + 1) * chunk] for k in range(pairs)]
    arrived = [mixed]
    for k in range(1, pairs):
        arrived.append(swap(jnp.concatenate(parts[k:] + parts[:k], axis=0), 2 * k))
    summed = functools.reduce(
        jnp.add, [mixed] + [jnp.concatenate([x[(pairs - k) * chunk :], x[: (pairs - k) * chunk]], axis=0) for k, x in enumerate(arrived) if k]
    )

    before = pl.pallas_call(
        stencil,
        out_shape=struct(fields.shape, f32),
        in_specs=[HBM] + [VMEM] * 6,
        out_specs=VMEM,
        scratch_shapes=[
            pltpu.VMEM(fields.shape, f32),
            pltpu.VMEM((cells // TILE, depth, LANES), f32),
            pltpu.SemaphoreType.DMA((cells // TILE,)),
        ],
        compiler_params=params(12),
        cost_estimate=cost(1 << 28, 1 << 23),
        name="stencil",
    )(in_hbm(fields), swirl_speed, ghost_mask, tile_flags, near, edge_low, edge_high)

    feed = pl.pallas_call(
        functools.partial(feed_rows, slots),
        out_shape=struct((cells * SUB + SUB, width), f32),
        in_specs=[SMEM] + [VMEM] * pairs,
        out_specs=VMEM,
        compiler_params=params(8),
        cost_estimate=cost(1 << 25, 1 << 20),
        name="feed",
    )(feed_target[0], *arrived)

    other = swap(summed, 1)

    return pl.pallas_call(
        functools.partial(finish, chunk, length),
        out_shape=struct(fields.shape, f32),
        in_specs=[VMEM] * 10,
        out_specs=HBM,
        scratch_shapes=[
            pltpu.VMEM((count * modes, width), f32),
            pltpu.VMEM((count, cells, width), f32),
            pltpu.VMEM(fields.shape, f32),
            pltpu.SemaphoreType.DMA((count, cells // SUB)),
        ],
        compiler_params=params(16),
        cost_estimate=cost(1 << 26, 1 << 23),
        name="finish",
    )(far, swirl_speed[0], axial_low, axial_high, row_top, summed, other, weights, feed, before)


def solution(mesh):
    return jax.shard_map(
        body,
        mesh=mesh,
        in_specs=(
            P(None, "azi", "ax", "rad"),
            P("azi", "ax", "rad"),
            P("azi", "ax", "rad"),
            P("azi", "ax"),
            P(),
            P("azi", None, None),
            P("azi", None, None, "rad"),
            P("azi", None, None),
        ),
        out_specs=P(None, "azi", "ax", "rad"),
        check_vma=False,
    )
```

```python
import functools
import math

import jax
import jax.numpy as jnp
from jax import lax
from jax.experimental import pallas as pl
from jax.experimental.pallas import tpu as pltpu
from jax.sharding import PartitionSpec as P


TILE = 16
HEAD = 4
LANES = 128
UNROLL = 8
SUB = 8
HIGH = lax.Precision.HIGHEST
VMEM = pl.BlockSpec(memory_space=pltpu.VMEM)
SMEM = pl.BlockSpec(memory_space=pltpu.SMEM)
HBM = pl.BlockSpec(memory_space=pltpu.HBM)
f32 = jnp.float32


def params(mib):
    return pltpu.CompilerParams(vmem_limit_bytes=mib << 20)


def cost(flops, size):
    return pl.CostEstimate(flops=flops, bytes_accessed=size, transcendentals=0)


def in_hbm(x):
    return pltpu.with_memory_space_constraint(x, pltpu.HBM)


def phases(length, first_cell, cell_count, mode_count):
    cells = first_cell + jnp.arange(cell_count, dtype=jnp.int32)
    order = jnp.arange(1, mode_count + 1, dtype=jnp.int32)
    angle = (order[:, None] * cells[None, :] % length).astype(f32) * (2.0 * math.pi / length)
    turned = (cells[:, None] * order[None, :] % length).astype(f32) * (2.0 * math.pi / length)
    return (
        jnp.concatenate([jnp.cos(angle), jnp.sin(angle)], axis=0),
        jnp.concatenate([jnp.cos(turned), jnp.sin(turned)], axis=1),
    )


def prepare(
    chunk, fields, phase, rates, profile, keep, send, shift, row_top, row_out, tile, rate, plenum, sem
):
    azi, ax = lax.axis_index("azi"), lax.axis_index("ax")
    last_ax = lax.axis_size("ax") - 1
    count, cells, depth, width = fields.shape
    sectors, slots, _ = profile.shape
    pairs = sectors // 2
    parity, place = azi % 2, azi // 2
    base = pairs * chunk
    t_pair = jnp.where(parity == 0, cells - 1, 0)
    t_shift = jnp.where(parity == 0, 0, cells - 1)
    row_sent = jnp.where((ax == 0) & (last_ax == 1), depth - 1, 0)
    first = pltpu.make_async_copy(fields.at[:, :, depth - 1, :], row_top, sem.at[0])
    first.start()
    copies = []
    for c in range(count):
        rows = slice(base + c * depth, base + (c + 1) * depth)
        copies.append(pltpu.make_async_copy(fields.at[c, t_pair], send.at[rows], sem.at[1 + 2 * c]))
        rows = slice(c * depth, (c + 1) * depth)
        copies.append(pltpu.make_async_copy(fields.at[c, t_shift], shift.at[rows], sem.at[2 + 2 * c]))
    for one in copies:
        one.start()
    face = pltpu.make_async_copy(fields.at[:, :, row_sent, :], row_out, sem.at[2 + 2 * count])
    face.start()
    for e, (block, _) in enumerate(columns_sent(width)):
        lanes = pl.ds(pl.multiple_of(block, LANES), LANES)
        copies.append(pltpu.make_async_copy(fields.at[:, :, :, lanes], tile.at[e], sem.at[5 + 2 * count + e]))
        copies[-1].start()
    supply = pltpu.make_async_copy(profile, plenum, sem.at[3 + 2 * count])
    supply.start()
    factor = pltpu.make_async_copy(rates, rate, sem.at[4 + 2 * count])
    factor.start()

    @pl.when(ax == last_ax)
    def _():
        first.wait()
        sums = [
            jnp.dot(phase[...], row_top[c], precision=HIGH, preferred_element_type=f32)
            for c in range(count)
        ]
        modes = phase.shape[0]
        length = count * modes // sectors
        blocks = []
        for s in range(sectors):
            c, m = divmod(s * length, modes)
            blocks.append(sums[c][m : m + length])
        for q in range(pairs):
            even, odd = blocks[2 * q], blocks[2 * q + 1]
            at = q * chunk
            keep[at : at + length] = jnp.where(parity == 0, even, odd)
            send[at : at + length] = jnp.where(parity == 0, odd, even)
            if chunk > length:
                keep[at + length : at + chunk] = jnp.zeros((chunk - length, width), f32)
                send[at + length : at + chunk] = jnp.zeros((chunk - length, width), f32)

    supply.wait()
    factor.wait()

    @pl.when(ax != last_ax)
    def _():
        first.wait()
        turned = rate[...].T
        for q in range(pairs):
            at = pl.multiple_of((q ^ place) * chunk, SUB)
            even = turned[:, 2 * q : 2 * q + 1] * plenum[2 * q]
            odd = turned[:, 2 * q + 1 : 2 * q + 2] * plenum[2 * q + 1]
            own = jnp.where(parity == 0, even, odd)
            other = jnp.where(parity == 0, odd, even)
            for p in range(2):
                rows = pl.ds(pl.multiple_of(at + p * slots, SUB), slots)
                keep[rows] = jnp.where(parity == p, own, 0.0)
                send[rows] = jnp.where(parity == p, other, 0.0)
            if chunk > 2 * slots:
                rest = pl.ds(pl.multiple_of(at + 2 * slots, SUB), chunk - 2 * slots)
                keep[rest] = jnp.zeros((chunk - 2 * slots, width), f32)
                send[rest] = jnp.zeros((chunk - 2 * slots, width), f32)

    for one in copies:
        one.wait()
    face.wait()


def columns_sent(width):
    if lax.axis_size("rad") != 2:
        return [(width - LANES, lambda j: (j + 1) % LANES), (0, lambda j: j)]
    more = jnp.where(lax.axis_index("rad") == 0, 1, 0)
    return [(more * (width - LANES), lambda j: (j + more) if j < LANES - 1 else j * (1 - more))]


def columns(tile, column):
    _, cells, depth = tile.shape[1:4]
    sides = columns_sent(LANES)
    lane = lax.broadcasted_iota(jnp.int32, (SUB, LANES), 1)
    halves = depth // SUB
    for e, (_, by) in enumerate(sides):
        for g in range(column.shape[1]):
            acc = jnp.zeros((SUB, LANES), f32)
            for j in range(LANES):
                c, rest = divmod(g * LANES + j, cells * halves)
                t, h = divmod(rest, halves)
                piece = tile[e, c, t, h * SUB : (h + 1) * SUB, :]
                acc = jnp.where(lane == j, pltpu.roll(piece, by(j), 1), acc)
            column[e, g] = acc


def stencil(source, swirl, mask, flags, near, column_low, column_high, final, out, fields, levels, sem, done):
    azi, rad = lax.axis_index("azi"), lax.axis_index("rad")
    last_rad = lax.axis_size("rad") - 1
    count, cells, depth, width = source.shape
    base = near.shape[0] - count * depth
    parity = azi % 2
    halves = depth // SUB
    blocks = width // LANES
    lane = lax.broadcasted_iota(jnp.int32, (SUB, LANES), 1)
    row = lax.broadcasted_iota(jnp.int32, (SUB, LANES), 0)
    at_left, at_right = lane == 0, lane == LANES - 1
    at_low, at_high = row == 0, row == SUB - 1
    has_left, has_right = rad > 0, rad < last_rad
    groups = cells // SUB

    def piece(k):
        begin, end = (k * SUB + 1 if k else 0), min(k * SUB + SUB + 1, cells)
        return pltpu.make_async_copy(source.at[:, begin:end], fields.at[:, begin + 1 : end + 1], sem.at[k])

    def ready(k):
        rows = pl.ds(k * SUB, SUB)
        return pltpu.make_async_copy(out.at[:, rows], final.at[:, rows], done.at[k])

    for k in range(groups):
        piece(k).start()
    for c in range(count):
        layer = near[base + c * depth : base + (c + 1) * depth]
        fields[c, 0] = jnp.where(parity == 1, layer, 0.0)
        fields[c, cells + 1] = jnp.where(parity == 0, layer, 0.0)
    turned = (0.5 * flags[...].astype(f32)).T
    for k in range(cells // TILE):
        levels[k] = jnp.broadcast_to(turned[:, k : k + 1], (depth, LANES))

    def cut(h, l):
        return slice(h * SUB, (h + 1) * SUB), slice(l * LANES, (l + 1) * LANES)

    def slab(t, carry):
        level = levels[t // TILE]
        for c in range(count):
            edges = []
            for h in range(halves):
                n = (c * cells + t) * halves + h
                g, j = n // LANES, n % LANES
                edges.append((
                    jnp.where(has_left, pltpu.roll(column_low[g], (LANES - j) % LANES, 1), 0.0),
                    jnp.where(has_right, pltpu.roll(column_high[g], LANES - 1 - j, 1), 0.0),
                ))
            parts = [[fields[(c, t + 1) + cut(h, l)] for l in range(blocks)] for h in range(halves)]
            ups = [[pltpu.roll(v, 1, 1) for v in p] for p in parts]
            downs = [[pltpu.roll(v, LANES - 1, 1) for v in p] for p in parts]
            for l in range(blocks):
                lows = [pltpu.roll(parts[h][l], 1, 0) for h in range(halves)]
                highs = [pltpu.roll(parts[h][l], SUB - 1, 0) for h in range(halves)]
                for h in range(halves):
                    left = jnp.where(at_left, ups[h][l - 1] if l else edges[h][0], ups[h][l])
                    right = jnp.where(at_right, downs[h][l + 1] if l + 1 < blocks else edges[h][1], downs[h][l])
                    low = jnp.where(at_low, lows[h - 1] if h else 0.0, lows[h])
                    high = jnp.where(at_high, highs[h + 1] if h + 1 < halves else 0.0, highs[h])
                    total = (left + right) + (low + high) + fields[(c, t + 2) + cut(h, l)]
                    speed = swirl[(t,) + cut(h, l)]
                    value = parts[h][l] * (0.4 - speed) + fields[(c, t) + cut(h, l)] * (speed + 0.1) + 0.1 * total
                    if c == 0:
                        out[(0, t) + cut(h, l)] = value
                    else:
                        live = jnp.where(mask[(t,) + cut(h, l)] == 0, level[h * SUB : (h + 1) * SUB], 0.0) * parts[h][l]
                        energy = fields[(0, t + 1) + cut(h, l)]
                        burn = live + live * jnp.tanh(2.0 * energy - 1.0)
                        out[(0, t) + cut(h, l)] += burn
                        out[(1, t) + cut(h, l)] = value - 0.5 * burn
        return carry

    def rows(k, carry):
        lax.fori_loop(0, SUB, lambda i, c: slab(k * SUB + i, c), 0, unroll=UNROLL)

        @pl.when(k < groups - 1)
        def _():
            ready(k).start()

        @pl.when(k < groups - 2)
        def _():
            begin = (k + 1) * SUB + 1
            source_rows, own_rows = pl.ds(begin, SUB), pl.ds(begin + 1, SUB)
            pltpu.make_async_copy(source.at[:, source_rows], fields.at[:, own_rows], sem.at[k + 1]).wait()

        @pl.when(k == groups - 2)
        def _():
            piece(groups - 1).wait()

        return carry

    piece(0).wait()
    lax.fori_loop(0, groups, rows, 0)
    for k in range(groups - 1):
        ready(k).wait()


def feed_rows(slots, targets, *refs):
    *arrived, feed = refs
    place = lax.axis_index("azi") // 2
    rows = feed.shape[0] - SUB
    feed[...] = jnp.zeros(feed.shape, f32)

    @pl.when(lax.axis_index("ax") == 0)
    def _():
        for k, block in enumerate(arrived):
            for p in range(2):
                for j in range(slots):
                    target = targets[2 * (place ^ k) + p, j]
                    at = jnp.where(target >= 0, target // HEAD * SUB + target % HEAD, rows)
                    r = p * slots + j
                    feed[pl.ds(at, 1), :] += block[r : r + 1, :]


def finish(chunk, length, far, speed, axial_low, axial_high, row_top, own, other, weights, feed, before, _, out, modes, high, result, sem):
    azi, ax = lax.axis_index("azi"), lax.axis_index("ax")
    last_ax = lax.axis_size("ax") - 1
    count, cells, depth, width = before.shape
    parity = azi % 2
    pairs = own.shape[0] // chunk

    @pl.when(ax == last_ax)
    def _():
        for k in range(pairs):
            for ref, p in ((own, parity), (other, 1 - parity)):
                at = pl.multiple_of((2 * k + p) * length, SUB)
                modes[pl.ds(at, length)] = ref[k * chunk : k * chunk + length]
        per = modes.shape[0] // count
        for c in range(count):
            rebuilt = jnp.dot(
                weights[c], modes[c * per : (c + 1) * per], precision=HIGH, preferred_element_type=f32
            )
            high[c] = 0.1 * row_top[c] - rebuilt

    @pl.when(ax != last_ax)
    def _():
        for c in range(count):
            high[c] = 0.1 * axial_high[c]

    scale = jnp.where(ax > 0, 0.1, 0.0)
    row = lax.broadcasted_iota(jnp.int32, (SUB, width), 0)
    group = SUB
    copies = []
    for b in range(cells // group):
        for c in range(count):
            low_rows = scale * axial_low[c, b * group : (b + 1) * group]
            high_rows = high[c, b * group : (b + 1) * group]
            for i in range(group):
                t = b * group + i
                head = before[c, t, :SUB] + jnp.where(row == 0, low_rows[i : i + 1], 0.0)
                if c == 1:
                    head = head + feed[t * SUB : (t + 1) * SUB]
                result[c, t, :SUB] = head
                if depth > 2 * SUB:
                    result[c, t, SUB : depth - SUB] = before[c, t, SUB : depth - SUB]
                tail = before[c, t, depth - SUB :]
                result[c, t, depth - SUB :] = tail + jnp.where(row == SUB - 1, high_rows[i : i + 1], 0.0)
                if t in (0, cells - 1):
                    layer = far[c * depth : (c + 1) * depth]
                    if t:
                        result[c, t] += jnp.where(parity == 1, 0.1 * layer, 0.0)
                    else:
                        result[c, t] += jnp.where(parity == 0, (speed[...] + 0.1) * layer, 0.0)
            at = slice(b * group, (b + 1) * group)
            if b in (0, cells // group - 1):
                parts = [slice(0, depth)]
            else:
                parts = [depth - 1, slice(0, HEAD) if c == 1 else 0]
            for k, part in enumerate(parts):
                copy = pltpu.make_async_copy(result.at[c, at, part], out.at[c, at, part], sem.at[c, b, k])
                copy.start()
                copies.append(copy)
    for copy in copies:
        copy.wait()


def body(fields, swirl_speed, ghost_mask, tile_flags, outlet_gain, feed_rate, plenum, feed_target):
    sectors, radials = lax.axis_size("azi"), lax.axis_size("rad")
    count, cells, depth, width = fields.shape
    half_modes = outlet_gain.shape[1]
    modes = 2 * half_modes
    slots = plenum.shape[2]
    length = count * modes // sectors
    chunk = max(length, 2 * slots)
    pairs = sectors // 2
    total_cells = cells * sectors
    phase, phase_t = phases(total_cells, lax.axis_index("azi") * cells, cells, half_modes)
    gain = jnp.concatenate([outlet_gain, outlet_gain], axis=1)
    weights = phase_t[None] * gain[:, None, :] * (0.1 * 2.0 / math.sqrt(half_modes * total_cells))
    groups = count * cells * depth // SUB // LANES

    struct = jax.ShapeDtypeStruct
    outer = 1 if radials == 2 else 2
    keep, send, shift, row_top, row_out, tile = pl.pallas_call(
        functools.partial(prepare, chunk),
        out_shape=(
            struct((pairs * chunk, width), f32),
            struct((pairs * chunk + count * depth, width), f32),
            struct((count * depth, width), f32),
            struct((count, cells, width), f32),
            struct((count, cells, width), f32),
            struct((outer, count, cells, depth, LANES), f32),
        ),
        in_specs=[HBM, VMEM, HBM, HBM],
        out_specs=[VMEM] * 6,
        scratch_shapes=[
            pltpu.VMEM((sectors, slots), f32),
            pltpu.VMEM((sectors, slots, width), f32),
            pltpu.SemaphoreType.DMA((2 * count + 7,)),
        ],
        compiler_params=params(12),
        cost_estimate=cost(1 << 26, 1 << 21),
        name="prepare",
    )(in_hbm(fields), phase, in_hbm(feed_rate[0]), in_hbm(plenum[0]))

    column = pl.pallas_call(
        columns,
        out_shape=struct((outer, groups, SUB, LANES), f32),
        in_specs=[VMEM],
        out_specs=VMEM,
        compiler_params=params(6),
        cost_estimate=cost(1 << 22, 1 << 19),
        name="columns",
    )(tile)

    def swap(x, k):
        return lax.ppermute(x, "azi", [(i, i ^ k) for i in range(sectors)])

    def across(axis, to_high, to_low, to_only):
        size = lax.axis_size(axis)
        if size == 2:
            received = lax.ppermute(to_only, axis, [(0, 1), (1, 0)])
            return received, received
        ups = [(i, i + 1) for i in range(size - 1)]
        return lax.ppermute(to_high, axis, ups), lax.ppermute(to_low, axis, [(b, a) for a, b in ups])

    offset = [(i, (i + 1) % sectors if i % 2 else (i - 1) % sectors) for i in range(sectors)]
    near = swap(send, 1)
    far = lax.ppermute(shift, "azi", offset)
    axial_low, axial_high = across("ax", row_top, row_out, row_out)
    edge_low, edge_high = across("rad", column[0], column[-1], column[0])

    mixed = keep + near[: pairs * chunk]
    parts = [mixed[k * chunk : (k + 1) * chunk] for k in range(pairs)]
    arrived = [mixed]
    for k in range(1, pairs):
        arrived.append(swap(jnp.concatenate(parts[k:] + parts[:k], axis=0), 2 * k))
    summed = functools.reduce(
        jnp.add, [mixed] + [jnp.concatenate([x[(pairs - k) * chunk :], x[: (pairs - k) * chunk]], axis=0) for k, x in enumerate(arrived) if k]
    )

    final, before = pl.pallas_call(
        stencil,
        out_shape=[struct(fields.shape, f32)] * 2,
        in_specs=[HBM] + [VMEM] * 6,
        out_specs=[HBM, VMEM],
        scratch_shapes=[
            pltpu.VMEM((count, cells + 2, depth, width), f32),
            pltpu.VMEM((cells // TILE, depth, LANES), f32),
            pltpu.SemaphoreType.DMA((cells // SUB,)),
            pltpu.SemaphoreType.DMA((cells // SUB,)),
        ],
        compiler_params=params(12),
        cost_estimate=cost(1 << 28, 1 << 23),
        name="stencil",
    )(in_hbm(fields), swirl_speed, ghost_mask, tile_flags, near, edge_low, edge_high)

    feed = pl.pallas_call(
        functools.partial(feed_rows, slots),
        out_shape=struct((cells * SUB + SUB, width), f32),
        in_specs=[SMEM] + [VMEM] * pairs,
        out_specs=VMEM,
        compiler_params=params(8),
        cost_estimate=cost(1 << 25, 1 << 20),
        name="feed",
    )(feed_target[0], *arrived)

    other = swap(summed, 1)

    return pl.pallas_call(
        functools.partial(finish, chunk, length),
        out_shape=struct(fields.shape, f32),
        in_specs=[VMEM] * 10 + [HBM],
        out_specs=HBM,
        input_output_aliases={10: 0},
        scratch_shapes=[
            pltpu.VMEM((count * modes, width), f32),
            pltpu.VMEM((count, cells, width), f32),
            pltpu.VMEM(fields.shape, f32),
            pltpu.SemaphoreType.DMA((count, cells // SUB, 2)),
        ],
        compiler_params=params(16),
        cost_estimate=cost(1 << 26, 1 << 23),
        name="finish",
    )(far, swirl_speed[0], axial_low, axial_high, row_top, summed, other, weights, feed, before, final)


def solution(mesh):
    return jax.shard_map(
        body,
        mesh=mesh,
        in_specs=(
            P(None, "azi", "ax", "rad"),
            P("azi", "ax", "rad"),
            P("azi", "ax", "rad"),
            P("azi", "ax"),
            P(),
            P("azi", None, None),
            P("azi", None, None, "rad"),
            P("azi", None, None),
        ),
        out_specs=P(None, "azi", "ax", "rad"),
        check_vma=False,
    )
```

```python
import functools
import math

import jax
import jax.numpy as jnp
from jax import lax
from jax.experimental import pallas as pl
from jax.experimental.pallas import tpu as pltpu
from jax.sharding import PartitionSpec as P


TILE = 16
HEAD = 4
LANES = 128
UNROLL = 8
SUB = 8
HIGH = lax.Precision.HIGHEST
VMEM = pl.BlockSpec(memory_space=pltpu.VMEM)
SMEM = pl.BlockSpec(memory_space=pltpu.SMEM)
HBM = pl.BlockSpec(memory_space=pltpu.HBM)
f32 = jnp.float32


def params(mib):
    return pltpu.CompilerParams(vmem_limit_bytes=mib << 20)


def cost(flops, size):
    return pl.CostEstimate(flops=flops, bytes_accessed=size, transcendentals=0)


def in_hbm(x):
    return pltpu.with_memory_space_constraint(x, pltpu.HBM)


def phases(length, first_cell, cell_count, mode_count):
    cells = first_cell + jnp.arange(cell_count, dtype=jnp.int32)
    order = jnp.arange(1, mode_count + 1, dtype=jnp.int32)
    angle = (order[:, None] * cells[None, :] % length).astype(f32) * (2.0 * math.pi / length)
    turned = (cells[:, None] * order[None, :] % length).astype(f32) * (2.0 * math.pi / length)
    return (
        jnp.concatenate([jnp.cos(angle), jnp.sin(angle)], axis=0),
        jnp.concatenate([jnp.cos(turned), jnp.sin(turned)], axis=1),
    )


def prepare(
    chunk, fields, phase, rates, profile, keep, send, shift, row_top, row_out, tile, rate, plenum, sem
):
    azi, ax = lax.axis_index("azi"), lax.axis_index("ax")
    last_ax = lax.axis_size("ax") - 1
    count, cells, depth, width = fields.shape
    sectors, slots, _ = profile.shape
    pairs = sectors // 2
    parity, place = azi % 2, azi // 2
    base = pairs * chunk
    t_pair = jnp.where(parity == 0, cells - 1, 0)
    t_shift = jnp.where(parity == 0, 0, cells - 1)
    row_sent = jnp.where((ax == 0) & (last_ax == 1), depth - 1, 0)
    first = pltpu.make_async_copy(fields.at[:, :, depth - 1, :], row_top, sem.at[0])
    first.start()
    supply = pltpu.make_async_copy(profile, plenum, sem.at[3 + 2 * count])
    supply.start()
    factor = pltpu.make_async_copy(rates, rate, sem.at[4 + 2 * count])
    factor.start()
    copies = []
    for c in range(count):
        rows = slice(base + c * depth, base + (c + 1) * depth)
        copies.append(pltpu.make_async_copy(fields.at[c, t_pair], send.at[rows], sem.at[1 + 2 * c]))
        rows = slice(c * depth, (c + 1) * depth)
        copies.append(pltpu.make_async_copy(fields.at[c, t_shift], shift.at[rows], sem.at[2 + 2 * c]))
    for one in copies:
        one.start()
    face = pltpu.make_async_copy(fields.at[:, :, row_sent, :], row_out, sem.at[2 + 2 * count])
    face.start()
    for e, (block, _) in enumerate(columns_sent(width)):
        lanes = pl.ds(pl.multiple_of(block, LANES), LANES)
        copies.append(pltpu.make_async_copy(fields.at[:, :, :, lanes], tile.at[e], sem.at[5 + 2 * count + e]))
        copies[-1].start()

    @pl.when(ax == last_ax)
    def _():
        first.wait()
        sums = [
            jnp.dot(phase[...], row_top[c], precision=HIGH, preferred_element_type=f32)
            for c in range(count)
        ]
        modes = phase.shape[0]
        length = count * modes // sectors
        blocks = []
        for s in range(sectors):
            c, m = divmod(s * length, modes)
            blocks.append(sums[c][m : m + length])
        for q in range(pairs):
            even, odd = blocks[2 * q], blocks[2 * q + 1]
            at = q * chunk
            keep[at : at + length] = jnp.where(parity == 0, even, odd)
            send[at : at + length] = jnp.where(parity == 0, odd, even)
            if chunk > length:
                keep[at + length : at + chunk] = jnp.zeros((chunk - length, width), f32)
                send[at + length : at + chunk] = jnp.zeros((chunk - length, width), f32)

    supply.wait()
    factor.wait()

    @pl.when(ax != last_ax)
    def _():
        first.wait()
        turned = rate[...].T
        for q in range(pairs):
            at = pl.multiple_of((q ^ place) * chunk, SUB)
            even = turned[:, 2 * q : 2 * q + 1] * plenum[2 * q]
            odd = turned[:, 2 * q + 1 : 2 * q + 2] * plenum[2 * q + 1]
            own = jnp.where(parity == 0, even, odd)
            other = jnp.where(parity == 0, odd, even)
            for p in range(2):
                rows = pl.ds(pl.multiple_of(at + p * slots, SUB), slots)
                keep[rows] = jnp.where(parity == p, own, 0.0)
                send[rows] = jnp.where(parity == p, other, 0.0)
            if chunk > 2 * slots:
                rest = pl.ds(pl.multiple_of(at + 2 * slots, SUB), chunk - 2 * slots)
                keep[rest] = jnp.zeros((chunk - 2 * slots, width), f32)
                send[rest] = jnp.zeros((chunk - 2 * slots, width), f32)

    for one in copies:
        one.wait()
    face.wait()


def columns_sent(width):
    if lax.axis_size("rad") != 2:
        return [(width - LANES, lambda j: (j + 1) % LANES), (0, lambda j: j)]
    more = jnp.where(lax.axis_index("rad") == 0, 1, 0)
    return [(more * (width - LANES), lambda j: (j + more) if j < LANES - 1 else j * (1 - more))]


def columns(tile, column):
    _, cells, depth = tile.shape[1:4]
    sides = columns_sent(LANES)
    lane = lax.broadcasted_iota(jnp.int32, (SUB, LANES), 1)
    halves = depth // SUB
    for e, (_, by) in enumerate(sides):
        for g in range(column.shape[1]):
            acc = jnp.zeros((SUB, LANES), f32)
            for j in range(LANES):
                c, rest = divmod(g * LANES + j, cells * halves)
                t, h = divmod(rest, halves)
                piece = tile[e, c, t, h * SUB : (h + 1) * SUB, :]
                acc = jnp.where(lane == j, pltpu.roll(piece, by(j), 1), acc)
            column[e, g] = acc


def stencil(source, swirl, mask, flags, near, column_low, column_high, final, out, fields, levels, sem, done):
    azi, rad = lax.axis_index("azi"), lax.axis_index("rad")
    last_rad = lax.axis_size("rad") - 1
    count, cells, depth, width = source.shape
    base = near.shape[0] - count * depth
    parity = azi % 2
    halves = depth // SUB
    blocks = width // LANES
    lane = lax.broadcasted_iota(jnp.int32, (SUB, LANES), 1)
    row = lax.broadcasted_iota(jnp.int32, (SUB, LANES), 0)
    at_left, at_right = lane == 0, lane == LANES - 1
    at_low, at_high = row == 0, row == SUB - 1
    has_left, has_right = rad > 0, rad < last_rad
    groups = cells // SUB

    def piece(k):
        begin, end = (k * SUB + 1 if k else 0), min(k * SUB + SUB + 1, cells)
        return pltpu.make_async_copy(source.at[:, begin:end], fields.at[:, begin + 1 : end + 1], sem.at[k])

    def ready(k):
        rows = pl.ds(k * SUB, SUB)
        return pltpu.make_async_copy(out.at[:, rows], final.at[:, rows], done.at[k])

    for k in range(groups):
        piece(k).start()
    for c in range(count):
        layer = near[base + c * depth : base + (c + 1) * depth]
        fields[c, 0] = jnp.where(parity == 1, layer, 0.0)
        fields[c, cells + 1] = jnp.where(parity == 0, layer, 0.0)
    turned = (0.5 * flags[...].astype(f32)).T
    for k in range(cells // TILE):
        levels[k] = jnp.broadcast_to(turned[:, k : k + 1], (depth, LANES))

    def cut(h, l):
        return slice(h * SUB, (h + 1) * SUB), slice(l * LANES, (l + 1) * LANES)

    def slab(t, carry):
        level = levels[t // TILE]
        for c in range(count):
            edges = []
            for h in range(halves):
                n = (c * cells + t) * halves + h
                g, j = n // LANES, n % LANES
                edges.append((
                    jnp.where(has_left, pltpu.roll(column_low[g], (LANES - j) % LANES, 1), 0.0),
                    jnp.where(has_right, pltpu.roll(column_high[g], LANES - 1 - j, 1), 0.0),
                ))
            parts = [[fields[(c, t + 1) + cut(h, l)] for l in range(blocks)] for h in range(halves)]
            ups = [[pltpu.roll(v, 1, 1) for v in p] for p in parts]
            downs = [[pltpu.roll(v, LANES - 1, 1) for v in p] for p in parts]
            for l in range(blocks):
                lows = [pltpu.roll(parts[h][l], 1, 0) for h in range(halves)]
                highs = [pltpu.roll(parts[h][l], SUB - 1, 0) for h in range(halves)]
                for h in range(halves):
                    left = jnp.where(at_left, ups[h][l - 1] if l else edges[h][0], ups[h][l])
                    right = jnp.where(at_right, downs[h][l + 1] if l + 1 < blocks else edges[h][1], downs[h][l])
                    low = jnp.where(at_low, lows[h - 1] if h else 0.0, lows[h])
                    high = jnp.where(at_high, highs[h + 1] if h + 1 < halves else 0.0, highs[h])
                    total = (left + right) + (low + high) + fields[(c, t + 2) + cut(h, l)]
                    speed = swirl[(t,) + cut(h, l)]
                    value = parts[h][l] * (0.4 - speed) + fields[(c, t) + cut(h, l)] * (speed + 0.1) + 0.1 * total
                    if c == 0:
                        out[(0, t) + cut(h, l)] = value
                    else:
                        live = jnp.where(mask[(t,) + cut(h, l)] == 0, level[h * SUB : (h + 1) * SUB], 0.0) * parts[h][l]
                        energy = fields[(0, t + 1) + cut(h, l)]
                        burn = live + live * jnp.tanh(2.0 * energy - 1.0)
                        out[(0, t) + cut(h, l)] += burn
                        out[(1, t) + cut(h, l)] = value - 0.5 * burn
        return carry

    def rows(k, carry):
        lax.fori_loop(0, SUB, lambda i, c: slab(k * SUB + i, c), 0, unroll=UNROLL)

        @pl.when(k < groups - 1)
        def _():
            ready(k).start()

        @pl.when(k < groups - 2)
        def _():
            begin = (k + 1) * SUB + 1
            source_rows, own_rows = pl.ds(begin, SUB), pl.ds(begin + 1, SUB)
            pltpu.make_async_copy(source.at[:, source_rows], fields.at[:, own_rows], sem.at[k + 1]).wait()

        @pl.when(k == groups - 2)
        def _():
            piece(groups - 1).wait()

        return carry

    piece(0).wait()
    lax.fori_loop(0, groups, rows, 0)
    for k in range(groups - 1):
        ready(k).wait()


def feed_rows(slots, targets, *refs):
    *arrived, feed = refs
    place = lax.axis_index("azi") // 2
    rows = feed.shape[0] - SUB
    feed[...] = jnp.zeros(feed.shape, f32)

    @pl.when(lax.axis_index("ax") == 0)
    def _():
        for k, block in enumerate(arrived):
            for p in range(2):
                for j in range(slots):
                    target = targets[2 * (place ^ k) + p, j]
                    at = jnp.where(target >= 0, target // HEAD * SUB + target % HEAD, rows)
                    r = p * slots + j
                    feed[pl.ds(at, 1), :] += block[r : r + 1, :]


def finish(chunk, length, far, speed, axial_low, axial_high, row_top, own, other, weights, feed, before, _, out, modes, high, result, sem):
    azi, ax = lax.axis_index("azi"), lax.axis_index("ax")
    last_ax = lax.axis_size("ax") - 1
    count, cells, depth, width = before.shape
    parity = azi % 2
    pairs = own.shape[0] // chunk

    @pl.when(ax == last_ax)
    def _():
        for k in range(pairs):
            for ref, p in ((own, parity), (other, 1 - parity)):
                at = pl.multiple_of((2 * k + p) * length, SUB)
                modes[pl.ds(at, length)] = ref[k * chunk : k * chunk + length]
        per = modes.shape[0] // count
        for c in range(count):
            rebuilt = jnp.dot(
                weights[c], modes[c * per : (c + 1) * per], precision=HIGH, preferred_element_type=f32
            )
            high[c] = 0.1 * row_top[c] - rebuilt

    @pl.when(ax != last_ax)
    def _():
        for c in range(count):
            high[c] = 0.1 * axial_high[c]

    scale = jnp.where(ax > 0, 0.1, 0.0)
    row = lax.broadcasted_iota(jnp.int32, (SUB, width), 0)
    group = SUB
    copies = []
    last = cells // group - 1
    for b in [last] + list(range(last)):
        for c in range(count):
            low_rows = scale * axial_low[c, b * group : (b + 1) * group]
            high_rows = high[c, b * group : (b + 1) * group]
            for i in range(group):
                t = b * group + i
                head = before[c, t, :SUB] + jnp.where(row == 0, low_rows[i : i + 1], 0.0)
                if c == 1:
                    head = head + feed[t * SUB : (t + 1) * SUB]
                result[c, t, :SUB] = head
                if depth > 2 * SUB:
                    result[c, t, SUB : depth - SUB] = before[c, t, SUB : depth - SUB]
                tail = before[c, t, depth - SUB :]
                result[c, t, depth - SUB :] = tail + jnp.where(row == SUB - 1, high_rows[i : i + 1], 0.0)
                if t in (0, cells - 1):
                    layer = far[c * depth : (c + 1) * depth]
                    if t:
                        result[c, t] += jnp.where(parity == 1, 0.1 * layer, 0.0)
                    else:
                        result[c, t] += jnp.where(parity == 0, (speed[...] + 0.1) * layer, 0.0)
            at = slice(b * group, (b + 1) * group)
            if b in (0, last):
                parts = [slice(0, depth)]
            else:
                parts = [depth - 1, slice(0, HEAD) if c == 1 else 0]
            for k, part in enumerate(parts):
                copy = pltpu.make_async_copy(result.at[c, at, part], out.at[c, at, part], sem.at[c, b, k])
                copy.start()
                copies.append(copy)
    for copy in copies:
        copy.wait()


def body(fields, swirl_speed, ghost_mask, tile_flags, outlet_gain, feed_rate, plenum, feed_target):
    sectors, radials = lax.axis_size("azi"), lax.axis_size("rad")
    count, cells, depth, width = fields.shape
    half_modes = outlet_gain.shape[1]
    modes = 2 * half_modes
    slots = plenum.shape[2]
    length = count * modes // sectors
    chunk = max(length, 2 * slots)
    pairs = sectors // 2
    total_cells = cells * sectors
    phase, phase_t = phases(total_cells, lax.axis_index("azi") * cells, cells, half_modes)
    gain = jnp.concatenate([outlet_gain, outlet_gain], axis=1)
    weights = phase_t[None] * gain[:, None, :] * (0.1 * 2.0 / math.sqrt(half_modes * total_cells))
    groups = count * cells * depth // SUB // LANES

    struct = jax.ShapeDtypeStruct
    outer = 1 if radials == 2 else 2
    keep, send, shift, row_top, row_out, tile = pl.pallas_call(
        functools.partial(prepare, chunk),
        out_shape=(
            struct((pairs * chunk, width), f32),
            struct((pairs * chunk + count * depth, width), f32),
            struct((count * depth, width), f32),
            struct((count, cells, width), f32),
            struct((count, cells, width), f32),
            struct((outer, count, cells, depth, LANES), f32),
        ),
        in_specs=[HBM, VMEM, HBM, HBM],
        out_specs=[VMEM] * 6,
        scratch_shapes=[
            pltpu.VMEM((sectors, slots), f32),
            pltpu.VMEM((sectors, slots, width), f32),
            pltpu.SemaphoreType.DMA((2 * count + 7,)),
        ],
        compiler_params=params(12),
        cost_estimate=cost(1 << 26, 1 << 21),
        name="prepare",
    )(in_hbm(fields), phase, in_hbm(feed_rate[0]), in_hbm(plenum[0]))

    column = pl.pallas_call(
        columns,
        out_shape=struct((outer, groups, SUB, LANES), f32),
        in_specs=[VMEM],
        out_specs=VMEM,
        compiler_params=params(6),
        cost_estimate=cost(1 << 22, 1 << 19),
        name="columns",
    )(tile)

    def swap(x, k):
        return lax.ppermute(x, "azi", [(i, i ^ k) for i in range(sectors)])

    def across(axis, to_high, to_low, to_only):
        size = lax.axis_size(axis)
        if size == 2:
            received = lax.ppermute(to_only, axis, [(0, 1), (1, 0)])
            return received, received
        ups = [(i, i + 1) for i in range(size - 1)]
        return lax.ppermute(to_high, axis, ups), lax.ppermute(to_low, axis, [(b, a) for a, b in ups])

    offset = [(i, (i + 1) % sectors if i % 2 else (i - 1) % sectors) for i in range(sectors)]
    near = swap(send, 1)
    far = lax.ppermute(shift, "azi", offset)
    axial_low, axial_high = across("ax", row_top, row_out, row_out)
    edge_low, edge_high = across("rad", column[0], column[-1], column[0])

    mixed = keep + near[: pairs * chunk]
    parts = [mixed[k * chunk : (k + 1) * chunk] for k in range(pairs)]
    arrived = [mixed]
    for k in range(1, pairs):
        arrived.append(swap(jnp.concatenate(parts[k:] + parts[:k], axis=0), 2 * k))
    summed = functools.reduce(
        jnp.add, [mixed] + [jnp.concatenate([x[(pairs - k) * chunk :], x[: (pairs - k) * chunk]], axis=0) for k, x in enumerate(arrived) if k]
    )

    final, before = pl.pallas_call(
        stencil,
        out_shape=[struct(fields.shape, f32)] * 2,
        in_specs=[HBM] + [VMEM] * 6,
        out_specs=[HBM, VMEM],
        scratch_shapes=[
            pltpu.VMEM((count, cells + 2, depth, width), f32),
            pltpu.VMEM((cells // TILE, depth, LANES), f32),
            pltpu.SemaphoreType.DMA((cells // SUB,)),
            pltpu.SemaphoreType.DMA((cells // SUB,)),
        ],
        compiler_params=params(12),
        cost_estimate=cost(1 << 28, 1 << 23),
        name="stencil",
    )(in_hbm(fields), swirl_speed, ghost_mask, tile_flags, near, edge_low, edge_high)

    feed = pl.pallas_call(
        functools.partial(feed_rows, slots),
        out_shape=struct((cells * SUB + SUB, width), f32),
        in_specs=[SMEM] + [VMEM] * pairs,
        out_specs=VMEM,
        compiler_params=params(8),
        cost_estimate=cost(1 << 25, 1 << 20),
        name="feed",
    )(feed_target[0], *arrived)

    other = swap(summed, 1)

    return pl.pallas_call(
        functools.partial(finish, chunk, length),
        out_shape=struct(fields.shape, f32),
        in_specs=[VMEM] * 10 + [HBM],
        out_specs=HBM,
        input_output_aliases={10: 0},
        scratch_shapes=[
            pltpu.VMEM((count * modes, width), f32),
            pltpu.VMEM((count, cells, width), f32),
            pltpu.VMEM(fields.shape, f32),
            pltpu.SemaphoreType.DMA((count, cells // SUB, 2)),
        ],
        compiler_params=params(16),
        cost_estimate=cost(1 << 26, 1 << 23),
        name="finish",
    )(far, swirl_speed[0], axial_low, axial_high, row_top, summed, other, weights, feed, before, final)


def solution(mesh):
    return jax.shard_map(
        body,
        mesh=mesh,
        in_specs=(
            P(None, "azi", "ax", "rad"),
            P("azi", "ax", "rad"),
            P("azi", "ax", "rad"),
            P("azi", "ax"),
            P(),
            P("azi", None, None),
            P("azi", None, None, "rad"),
            P("azi", None, None),
        ),
        out_specs=P(None, "azi", "ax", "rad"),
        check_vma=False,
    )
```
